256 devices in a mesh: gx: 8 (over y, core), gy: 4 (over x), gz: 8 (over z).
Axes of the slice: x: 4, y: 4, z: 8, core: 2. Of those that a mesh axis runs over, the one named last changes fastest.
Arguments:
- positions: float32 [3, 32, 16, 1024], P(None, 'gx', 'gy', 'gz'), may hold values from 0 to 1
- charges: float32 [32, 16, 1024], P('gx', 'gy', 'gz'), may hold values from -1.2 to 1.2
- counts: int32 [32, 16, 32], P('gx', 'gy', 'gz'), may hold values from 16 to 32
- moment_shift: bfloat16 [8, 81, 81], replicated, may hold values from -0.25 to 0.25
- far_operators: bfloat16 [81, 25600], replicated, may hold values from -0.046875 to 0.046875
- local_shift: bfloat16 [8, 81, 81], replicated, may hold values from -0.625 to 0.625
- lattice_operator: bfloat16 [81, 81], replicated, may hold values from -0.625 to 0.625
Outputs:
- potential: float32 [32, 16, 1024], P('gx', 'gy', 'gz')
- electric_field: float32 [3, 32, 16, 1024], P(None, 'gx', 'gy', 'gz')
The draws below stay inside these ranges and needn't reach their ends.
Inputs may be any that keep to these rules, and one draw needn't show every extreme that they name: `counts`: number of live charges in each leaf; slots at or past it are pads.
All inputs are finite; a program needn't handle non-finite values.
Results may differ from the reference program's by a relative error of at most 0.00035.
Values sent between devices are 32-bit elements; how exact they have to be, the bound alone decides.
No kernel may reach another device: no remote copies, remote signals or barrier semaphores. Data moves between devices by JAX's collectives and lax.ppermute only.
A program may use at most 256 MiB of HBM per device.

```python
import jax
import jax.numpy as jnp
import numpy as np
from jax import lax

ORDER = 8
TERMS = 81
SLOTS = 32
OPERATOR_COLUMNS = 25600
GRID_X = 32
GRID_Y = 16
GRID_Z = 32


def touch_ends(entries, own_key, least, top_value):
    shape = entries.shape
    spot = [jax.random.randint(jax.random.fold_in(own_key, axis), (), 0, shape[axis]) for axis in range(len(shape))]
    entries = entries.at[tuple(spot)].set(least)
    longest = shape.index(max(shape))
    spot[longest] = (spot[longest] + 1) % shape[longest]
    return entries.at[tuple(spot)].set(top_value)


def block_levels(own_key, dims, shards, least, top_value):
    gain = 1.0
    for axis_at, blocks in shards:
        steps = jax.random.uniform(jax.random.fold_in(jax.random.fold_in(own_key, 6), axis_at), (blocks,), jnp.float32, least / len(shards), top_value / len(shards))
        gain = gain * jnp.repeat(jnp.exp(steps), dims[axis_at] // blocks).reshape((-1,) + (1,) * (len(dims) - 1 - axis_at))
    return gain


def bell_draw(rng, shape, deviation, most, split=(), kind=jnp.bfloat16):
    drawn = jax.random.normal(rng, shape, jnp.float32) * deviation
    if len(split) > 0:
        drawn = block_levels(rng, shape, split, -0.22, 0.18) * drawn
    return jnp.clip(drawn, min=-most, max=most).astype(kind)


def setup_inputs(seed: int = 0) -> dict:
    seeds = jax.random.split(jax.random.key(seed), 8)
    return {
        "positions": jnp.clip(1.0 * jax.random.uniform(seeds[0], (3, GRID_X, GRID_Y, GRID_Z * SLOTS), jnp.float32) ** block_levels(seeds[0], (3, GRID_X, GRID_Y, GRID_Z * SLOTS), ((1, 8), (2, 4), (3, 8)), -0.2, 0.2), 0.0, 1.0),
        "charges": bell_draw(seeds[1], (GRID_X, GRID_Y, GRID_Z * SLOTS), 0.2, 1.2, ((0, 8), (1, 4), (2, 8)), jnp.float32),
        "counts": touch_ends(jax.random.randint(seeds[2], (GRID_X, GRID_Y, GRID_Z), SLOTS // 2, SLOTS + 1), jax.random.fold_in(seeds[2], 1), SLOTS // 2, SLOTS).astype(jnp.int32),
        "moment_shift": bell_draw(seeds[3], (8, TERMS, TERMS), (8 * TERMS) ** -0.5, 0.25),
        "far_operators": bell_draw(seeds[4], (TERMS, OPERATOR_COLUMNS), (189 * TERMS) ** -0.5, 0.046875),
        "local_shift": bell_draw(seeds[5], (8, TERMS, TERMS), TERMS ** -0.5, 0.625),
        "lattice_operator": bell_draw(seeds[6], (TERMS, TERMS), TERMS ** -0.5, 0.625),
    }


SOFTENING = 0.0625

def offset_table():
    listed = []
    for shift_x in range(-3, 4):
        for shift_y in range(-3, 4):
            for shift_z in range(-3, 4):
                if max(abs(shift_x), abs(shift_y), abs(shift_z)) >= 2:
                    listed.append((shift_x, shift_y, shift_z))
    return np.array(listed, dtype=np.int32)

def exponent_table(degree):
    listed = []
    for accumulated in range(degree + 1):
        for height in (0, 1):
            for power_x in range(accumulated - height + 1):
                listed.append((power_x, accumulated - height - power_x, height))
    return np.array(listed, dtype=np.int32)

def power_stack(values, degree):
    listed = [jnp.ones_like(values)]
    for exponent in range(degree):
        listed.append(listed[-1] * values)
    return jnp.stack(listed)

def slope_stack(powers, degree):
    listed = [jnp.zeros_like(powers[0])]
    for exponent in range(1, degree + 1):
        listed.append(float(exponent) * powers[exponent - 1])
    return jnp.stack(listed)

def monomials(relative, degree, with_slopes):
    centred = relative - 0.5
    exponents = exponent_table(degree)
    powers_x = power_stack(centred[0], degree)
    powers_y = power_stack(centred[1], degree)
    powers_z = power_stack(centred[2], degree)
    part_x = powers_x[exponents[:, 0]]
    part_y = powers_y[exponents[:, 1]]
    part_z = powers_z[exponents[:, 2]]
    values = part_x * part_y * part_z
    if not with_slopes:
        return (values, None)
    slope_x = slope_stack(powers_x, degree)[exponents[:, 0]]
    slope_y = slope_stack(powers_y, degree)[exponents[:, 1]]
    slope_z = slope_stack(powers_z, degree)[exponents[:, 2]]
    slopes = (slope_x * part_y * part_z, part_x * slope_y * part_z, part_x * part_y * slope_z)
    return (values, slopes)

def to_moments(stacked):
    values = monomials(stacked[:3], ORDER, False)[0]
    return lax.optimization_barrier(jnp.sum(values * stacked[3][None], axis=-1))

def moments_up(child, operators):
    term_count, size_x, size_y, size_z = child.shape
    grouped = child.reshape(term_count, size_x // 2, 2, size_y // 2, 2, size_z // 2, 2)
    accumulated = jnp.zeros((term_count, size_x // 2 * (size_y // 2) * (size_z // 2)), jnp.float32)
    for octant in range(8):
        child_piece = grouped[:, :, octant >> 2 & 1, :, octant >> 1 & 1, :, octant & 1].reshape(term_count, -1)
        accumulated = accumulated + jnp.dot(operators[octant], child_piece, precision=lax.Precision.HIGHEST)
    return accumulated.reshape(term_count, size_x // 2, size_y // 2, size_z // 2)

def locals_down(parent, operators):
    term_count, size_x, size_y, size_z = parent.shape
    flat_parent = parent.reshape(term_count, -1)
    pieces = [jnp.dot(operators[octant], flat_parent, precision=lax.Precision.HIGHEST).reshape(term_count, size_x, size_y, size_z) for octant in range(8)]
    stacked = jnp.stack(pieces, axis=1).reshape(term_count, 2, 2, 2, size_x, size_y, size_z)
    return stacked.transpose(0, 4, 1, 5, 2, 6, 3).reshape(term_count, 2 * size_x, 2 * size_y, 2 * size_z)

def far_terms(source, grid_shape, coords, parity, operators):
    shifts = offset_table()
    offset_count = shifts.shape[0]
    term_count = source.shape[0]
    shift_x = jnp.asarray(shifts[:, 0:1])
    shift_y = jnp.asarray(shifts[:, 1:2])
    shift_z = jnp.asarray(shifts[:, 2:3])
    size_x, size_y, size_z = grid_shape
    coord_x, coord_y, coord_z = coords
    flat_index = ((coord_x[None, :] + shift_x) % size_x * size_y + (coord_y[None, :] + shift_y) % size_y) * size_z + (coord_z[None, :] + shift_z) % size_z
    picked = jnp.take(source, flat_index, axis=1)
    if parity is not None:
        odd_x, odd_y, odd_z = parity
        admitted = (shift_x >= -2 - odd_x[None, :]) & (shift_x <= 3 - odd_x[None, :])
        admitted = admitted & (shift_y >= -2 - odd_y[None, :]) & (shift_y <= 3 - odd_y[None, :])
        admitted = admitted & (shift_z >= -2 - odd_z[None, :]) & (shift_z <= 3 - odd_z[None, :])
        picked = picked * admitted.astype(jnp.float32)[None]
    ordered = jnp.transpose(picked, (1, 0, 2)).reshape(offset_count * term_count, -1)
    return jnp.dot(operators[:, :offset_count * term_count], ordered, precision=lax.Precision.HIGHEST)

def level_terms(moments, restrict, operators):
    term_count, size_x, size_y, size_z = moments.shape
    target_count = size_x * size_y * size_z
    block_size = min(target_count, 512)
    blocks = jnp.arange(target_count, dtype=jnp.int32).reshape(target_count // block_size, block_size)
    source = moments.reshape(term_count, target_count)

    def one_block(block_rows):
        coord_x = block_rows // (size_y * size_z)
        coord_y = block_rows // size_z % size_y
        coord_z = block_rows % size_z
        parity = (coord_x % 2, coord_y % 2, coord_z % 2) if restrict else None
        return far_terms(source, (size_x, size_y, size_z), (coord_x, coord_y, coord_z), parity, operators)
    result = lax.map(one_block, blocks)
    return result.transpose(1, 0, 2).reshape(term_count, size_x, size_y, size_z)

def evaluate(extended, slab_local, live_mask):
    term_count, size_x, size_y, size_z = slab_local.shape
    slot_count = extended.shape[4]
    target = extended[:, 1:size_x + 1, 1:size_y + 1, 1:size_z + 1, :]
    self_mask = (1.0 - jnp.eye(slot_count, dtype=jnp.float32))[:, None, None, None, :]
    near_potential = jnp.zeros((size_x, size_y, size_z, slot_count), jnp.float32)
    near_x = jnp.zeros_like(near_potential)
    near_y = jnp.zeros_like(near_potential)
    near_z = jnp.zeros_like(near_potential)
    for shift_x in (-1, 0, 1):
        for shift_y in (-1, 0, 1):
            for shift_z in (-1, 0, 1):
                source = extended[:, 1 + shift_x:1 + shift_x + size_x, 1 + shift_y:1 + shift_y + size_y, 1 + shift_z:1 + shift_z + size_z, :]
                source = jnp.moveaxis(source, 4, 1)[..., None]
                delta_x = target[0][None] - source[0] - float(shift_x)
                delta_y = target[1][None] - source[1] - float(shift_y)
                delta_z = target[2][None] - source[2] - float(shift_z)
                distance = delta_x * delta_x + delta_y * delta_y + delta_z * delta_z + SOFTENING
                inverse = lax.rsqrt(distance)
                weight = source[3] * inverse
                if shift_x == 0 and shift_y == 0 and (shift_z == 0):
                    weight = weight * self_mask
                near_potential = near_potential + lax.optimization_barrier(jnp.sum(weight, axis=0))
                cubic_weight = weight * inverse * inverse
                near_x = near_x + lax.optimization_barrier(jnp.sum(cubic_weight * delta_x, axis=0))
                near_y = near_y + lax.optimization_barrier(jnp.sum(cubic_weight * delta_y, axis=0))
                near_z = near_z + lax.optimization_barrier(jnp.sum(cubic_weight * delta_z, axis=0))
    values, slopes = monomials(target[:3], ORDER, True)
    expanded = slab_local[..., None]
    potential = (near_potential + lax.optimization_barrier(jnp.sum(expanded * values, axis=0))) * live_mask
    field_out = jnp.stack([near_x - lax.optimization_barrier(jnp.sum(expanded * slopes[0], axis=0)), near_y - lax.optimization_barrier(jnp.sum(expanded * slopes[1], axis=0)), near_z - lax.optimization_barrier(jnp.sum(expanded * slopes[2], axis=0))]) * live_mask[None]
    return (potential, field_out)

def reference(positions, charges, counts, moment_shift, far_operators, local_shift, lattice_operator):
    slots_index = jnp.arange(SLOTS, dtype=jnp.int32)
    live_mask = (slots_index[None, None, None, :] < counts[..., None]).astype(jnp.float32)
    weights = charges.reshape(GRID_X, GRID_Y, GRID_Z, SLOTS) * live_mask
    stacked = jnp.concatenate([positions.reshape(3, GRID_X, GRID_Y, GRID_Z, SLOTS), weights[None]], axis=0)
    upward = moment_shift.astype(jnp.float32)
    across = far_operators.astype(jnp.float32)
    downward = local_shift.astype(jnp.float32)
    lattice = lattice_operator.astype(jnp.float32)
    moments_leaf = jnp.moveaxis(lax.map(to_moments, jnp.moveaxis(stacked, 1, 0)), 0, 1)
    moments_mid = moments_up(moments_leaf, upward)
    moments_upper = moments_up(moments_mid, upward)
    moments_top = moments_up(moments_upper, upward)
    term_count = moments_top.shape[0]
    root_moments = lax.optimization_barrier(jnp.sum(moments_top.reshape(term_count, -1), axis=1))
    lattice_term = jnp.dot(lattice, root_moments[:, None], precision=lax.Precision.HIGHEST).reshape(term_count, 1, 1, 1)
    local_top = 0.125 * (level_terms(moments_top, False, across) + lattice_term)
    local_upper = 0.25 * level_terms(moments_upper, True, across) + locals_down(local_top, downward)
    local_mid = 0.5 * level_terms(moments_mid, True, across) + locals_down(local_upper, downward)
    local_leaf = level_terms(moments_leaf, True, across) + locals_down(local_mid, downward)
    padded = jnp.pad(stacked, ((0, 0), (1, 1), (1, 1), (1, 1), (0, 0)), mode='wrap')

    def one_slab(slab_row):
        extended = lax.dynamic_slice_in_dim(padded, slab_row, 3, axis=1)
        slab_local = lax.dynamic_slice_in_dim(local_leaf, slab_row, 1, axis=1)
        slab_live = lax.dynamic_slice_in_dim(live_mask, slab_row, 1, axis=0)
        return evaluate(extended, slab_local, slab_live)
    potential, field_out = lax.map(one_slab, jnp.arange(GRID_X, dtype=jnp.int32))
    potential = potential.reshape(GRID_X, GRID_Y, GRID_Z * SLOTS)
    field_out = jnp.moveaxis(field_out, 0, 1).reshape(3, GRID_X, GRID_Y, GRID_Z * SLOTS)
    return (potential, field_out)
```

```python
import jax
import jax.numpy as jnp
import numpy as np
from jax import lax
from jax.experimental import pallas as pl
from jax.experimental.pallas import tpu as pltpu
from jax.sharding import PartitionSpec as P

ORDER = 8
TERMS = 81
SLOTS = 32
SOFTENING = 0.0625
LANES = 128
OFFSETS = 343
PLANE = 49 * LANES
F32 = jnp.float32
BF16 = jnp.bfloat16


def exponent_table():
    listed = []
    for accumulated in range(ORDER + 1):
        for height in (0, 1):
            for power_x in range(accumulated - height + 1):
                listed.append((power_x, accumulated - height - power_x, height))
    return listed


EXPONENTS = exponent_table()


def offset_rows():
    rows, count = [], 0
    for x in range(-3, 4):
        for y in range(-3, 4):
            for z in range(-3, 4):
                if max(abs(x), abs(y), abs(z)) >= 2:
                    rows.append(count)
                    count += 1
                else:
                    rows.append(-1)
    return rows


OFFSET_ROWS = offset_rows()


def gradient_tables():
    place = {e: k for k, e in enumerate(EXPONENTS)}
    tables = np.zeros((3, LANES, LANES), np.float32)
    for k, e in enumerate(EXPONENTS):
        for axis in range(3):
            if e[axis] > 0:
                lowered = list(e)
                lowered[axis] -= 1
                tables[axis, k, place[tuple(lowered)]] = e[axis]
    return tables


def full_spec(shape):
    return pl.BlockSpec(shape, lambda *_: (0,) * len(shape))


def nt_dot(left, right):
    return lax.dot_general(left, right, (((1,), (1,)), ((), ())), preferred_element_type=F32)


def split(value):
    upper = value.astype(BF16)
    lower = (value - upper.astype(F32)).astype(BF16)
    return upper, lower


def stack_split(value):
    upper = value.astype(BF16).astype(F32)
    return jnp.concatenate([upper, value - upper], axis=0).astype(BF16)


def apply_op(value, operator):
    both = nt_dot(stack_split(value)[:, :TERMS], operator)
    return both[:8] + both[8:]


def unpack_octants(source_ref, rows):
    rows[:, 0:TERMS] = source_ref[...].astype(F32).reshape(8 * TERMS, TERMS)


def octant_operator(rows, octant):
    return rows[pl.ds(octant, TERMS, stride=8), :][:, :TERMS].astype(BF16)


def iota(shape, axis):
    return lax.broadcasted_iota(jnp.int32, shape, axis)


def powers(value):
    listed = [None, value]
    for _ in range(2, ORDER + 1):
        listed.append(listed[-1] * value)
    return listed


def write_monomials(target, positions, factor):
    px = powers(positions[0] - 0.5)
    py = powers(positions[1] - 0.5)
    pz = positions[2] - 0.5
    for k, (a, b, c) in enumerate(EXPONENTS):
        value = factor
        if a:
            value = px[a] if value is None else value * px[a]
        if b:
            value = py[b] if value is None else value * py[b]
        if c:
            value = pz if value is None else value * pz
        if value is None:
            value = jnp.ones_like(pz)
        target[k * 16 : (k + 1) * 16, :] = value
    target[TERMS * 16 : LANES * 16, :] = jnp.zeros(((LANES - TERMS) * 16, LANES), F32)


def moments_kernel(
    pos_hbm,
    charge_hbm,
    count_hbm,
    shift_hbm,
    comb_ref,
    low_ref,
    high_ref,
    upper_ref,
    alone_ref,
    live_ref,
    pos_ref,
    charge_ref,
    count_ref,
    shift_ref,
    mono,
    leaf,
    rows,
    sems,
):
    loads = [
        pltpu.make_async_copy(a, b, sems.at[n])
        for n, (a, b) in enumerate(
            (
                (count_hbm, count_ref),
                (charge_hbm, charge_ref),
                (pos_hbm, pos_ref),
                (shift_hbm, shift_ref),
            )
        )
    ]
    for load in loads:
        load.start()
    for load in loads[:3]:
        load.wait()
    lane = iota((16, LANES), 1)
    count = jnp.zeros((16, LANES), jnp.int32)
    for z in range(4):
        count = jnp.where(lane // SLOTS == z, count_ref[:, z : z + 1], count)
    live = (lane % SLOTS < count).astype(F32)
    live_ref[...] = live
    weight = charge_ref[...] * live
    write_monomials(mono, (pos_ref[0], pos_ref[1], pos_ref[2]), weight)
    uppers, lowers = [], []
    for row in range(16):
        high, low = split(mono[pl.ds(row, LANES, stride=16), :])
        uppers.append(high)
        lowers.append(low)
    row = iota((64, 2048), 0)
    x = (row >> 5 & 1) * 2 + (row >> 2 & 1)
    y = (row >> 4 & 1) * 2 + (row >> 1 & 1)
    z = (row >> 3 & 1) * 2 + (row & 1)
    picker = (iota((64, 2048), 1) // SLOTS == (x * 4 + y) * 4 + z).astype(F32).astype(BF16)
    moments = nt_dot(picker, jnp.concatenate(uppers, axis=1)) + nt_dot(
        picker, jnp.concatenate(lowers, axis=1)
    )
    leaf[...] = moments
    comb_ref[:, 8:16, :] = moments.reshape(8, 8, LANES)
    lane8 = iota((8, LANES), 1)
    index = (iota((8, LANES), 0) % 4) * SLOTS + lane8 % SLOTS
    for xy in range(16):
        pieces = [pos_ref[c, xy : xy + 1, :] for c in range(3)] + [weight[xy : xy + 1, :]]
        merged = None
        for c, piece in enumerate(pieces):
            moved = jnp.take_along_axis(jnp.broadcast_to(piece, (8, LANES)), index, axis=1)
            merged = moved if merged is None else jnp.where(lane8 // SLOTS == c, moved, merged)
        cx, cy = xy // 4, xy % 4
        for half in range(2):
            parent = (cx // 2) * 4 + (cy // 2) * 2 + half
            inner = (cx % 2) * 4 + (cy % 2) * 2
            comb_ref[parent, inner : inner + 2, :] = merged[2 * half : 2 * half + 2, :]
    loads[3].wait()
    unpack_octants(shift_ref, rows)
    operators = [octant_operator(rows, octant) for octant in range(8)]
    upper_ref[...] = jnp.zeros((8, LANES), F32)
    middle = jnp.zeros((8, TERMS), F32)
    for octant in range(8):
        middle = middle + apply_op(leaf[pl.ds(octant, 8, stride=8), :], operators[octant])
    upper_ref[0:8, 0:TERMS] = middle
    wide = upper_ref[...]
    total = jnp.zeros((8, TERMS), F32)
    row8 = iota((8, TERMS), 0)
    for octant in range(8):
        total = total + jnp.where(row8 == octant, apply_op(wide, operators[octant]), 0.0)
    alone_ref[...] = jnp.zeros((8, LANES), F32)
    alone_ref[0:1, 0:TERMS] = jnp.sum(total, axis=0, keepdims=True)
    for half, target in enumerate((low_ref, high_ref)):
        for bx in range(2):
            for bz in range(2):
                at = 16 * (2 * bx + bz)
                target[at : at + 16, :] = comb_ref[4 * bx + 2 * half + bz]
        target[64:72, :] = upper_ref[...]
        target[72:80, :] = alone_ref[...]


def make_moments():
    return pl.pallas_call(
        moments_kernel,
        out_shape=(
            jax.ShapeDtypeStruct((8, 16, LANES), F32),
            jax.ShapeDtypeStruct((80, LANES), F32),
            jax.ShapeDtypeStruct((80, LANES), F32),
            jax.ShapeDtypeStruct((8, LANES), F32),
            jax.ShapeDtypeStruct((8, LANES), F32),
            jax.ShapeDtypeStruct((16, LANES), F32),
        ),
        in_specs=[pl.BlockSpec(memory_space=pl.ANY)] * 4,
        scratch_shapes=[
            pltpu.VMEM((3, 16, LANES), F32),
            pltpu.VMEM((16, LANES), F32),
            pltpu.VMEM((16, 4), jnp.int32),
            pltpu.VMEM((TERMS, 8, TERMS), BF16),
            pltpu.VMEM((LANES * 16, LANES), F32),
            pltpu.VMEM((64, LANES), F32),
            pltpu.VMEM((8 * TERMS, LANES), F32),
            pltpu.SemaphoreType.DMA((4,)),
        ],
        name="moments",
    )


UPPER_ROWS = 768
CUTS = [-(-row * TERMS // LANES) * LANES for row in (0, 49, 98, 138, 178, 218, 267)] + [25600]


def spot(relative_x, relative_z, relative_y):
    x = (relative_x + 3 & 7) + 1
    z = (relative_z + 3 & 7) + 1
    xb = x * 11 >> 5
    zb = z * 11 >> 5
    return xb * 216 + zb * 72 + (x - 3 * xb) * 24 + (z - 3 * zb) * 8 + (relative_y + 1 & 3)


def write_hot(target, column):
    rows = column.shape[0]
    lane = iota((rows, LANES), 1)
    for block in range(UPPER_ROWS // LANES):
        hot = (lane + block * LANES == column).astype(F32).astype(BF16)
        target[:, block * LANES : (block + 1) * LANES] = hot


def widen(far_hbm, wide_hbm, far_ref, wide_ref, sems, first, last):
    start = max(CUTS[first] - LANES, 0)
    edges = [start] + CUTS[first + 1 : last + 1]
    count = last - first
    loads = []
    for p in range(count):
        size = edges[p + 1] - edges[p]
        loads.append(
            pltpu.make_async_copy(
                far_hbm.at[:, pl.ds(edges[p], size)], far_ref.at[:, pl.ds(edges[p] - start, size)], sems.at[p]
            )
        )
    stores = [pltpu.make_async_copy(wide_ref.at[p], wide_hbm.at[p], sems.at[count + p]) for p in range(count)]
    for load in loads:
        load.start()

    def finish():
        lane = iota((TERMS, LANES), 1)
        for slot in range(49 * first, 49 * last):
            source = OFFSET_ROWS[slot]
            plane, inside = slot // 49 - first, slot % 49
            if inside == 0:
                loads[plane].wait()
            span = slice(inside * LANES, (inside + 1) * LANES)
            if source < 0:
                wide_ref[plane, :, span] = jnp.zeros((TERMS, LANES), BF16)
            else:
                base, shift = divmod(source * TERMS - start, LANES)
                merged = far_ref[:, base * LANES : (base + 1) * LANES]
                if shift + TERMS > LANES:
                    following = far_ref[:, (base + 1) * LANES : (base + 2) * LANES]
                    merged = jnp.where(lane >= shift, merged.astype(F32), following.astype(F32))
                    merged = merged.astype(BF16)
                if shift:
                    merged = pltpu.roll(merged, LANES - shift, 1)
                wide_ref[plane, :, span] = merged
            if inside == 48:
                stores[plane].start()
        for store in stores:
            store.wait()

    return finish


SPLIT = 4
WIDTHS = (CUTS[SPLIT], 25600 - CUTS[SPLIT] + LANES)


def first_kernel(far_hbm, after_ref, wide_hbm, far_ref, wide_ref, sems):
    widen(far_hbm, wide_hbm, far_ref, wide_ref, sems, 0, SPLIT)()


def second_kernel(
    index_ref,
    far_hbm,
    pos_ref,
    after_ref,
    wide_hbm,
    value_hbm,
    upper_hbm,
    child_hbm,
    far_ref,
    wide_ref,
    value_ref,
    upper_ref,
    child_ref,
    mono,
    sems,
):
    finish = widen(far_hbm, wide_hbm, far_ref, wide_ref, sems, SPLIT, 7)
    parity_x, parity_y, parity_z = index_ref[0], index_ref[1], index_ref[2]
    row = iota((256, LANES), 0)
    octant, box = row >> 5, row & 31
    vx = 2 * (box >> 3) + (octant >> 2) - parity_x
    vy = 2 * (box >> 2 & 1) + (octant >> 1 & 1) - parity_y
    vz = 2 * (box & 3) + (octant & 1) - parity_z
    write_hot(child_ref, spot(vx, vz, vy))
    row = iota((344, LANES), 0)
    plane = row * 1338 >> 16
    inside = row - plane * 49
    line = inside * 37 >> 8
    dx, dy, dz = plane - 3, line - 3, inside - line * 7 - 3
    fine = (dx >= -2 - parity_x) & (dx <= 3 - parity_x)
    fine = fine & (dy >= -2 - parity_y) & (dy <= 3 - parity_y)
    fine = fine & (dz >= -2 - parity_z) & (dz <= 3 - parity_z)
    write_hot(upper_ref, jnp.where(fine, spot(dx, dz, dy), -1))
    write_monomials(mono, (pos_ref[0], pos_ref[1], pos_ref[2]), None)
    for row in range(16):
        high, low = split(mono[pl.ds(row, LANES, stride=16), :])
        value_ref[0, :, row * LANES : (row + 1) * LANES] = high
        value_ref[1, :, row * LANES : (row + 1) * LANES] = low
    outs = [
        pltpu.make_async_copy(a, b, sems.at[2 * (7 - SPLIT) + n])
        for n, (a, b) in enumerate(((value_ref, value_hbm), (upper_ref, upper_hbm), (child_ref, child_hbm)))
    ]
    for out in outs:
        out.start()
    finish()
    for out in outs:
        out.wait()


VMEM_SPEC = pl.BlockSpec(memory_space=pltpu.VMEM)
HBM_SPEC = pl.BlockSpec(memory_space=pl.ANY)
SMEM_SPEC = pl.BlockSpec(memory_space=pltpu.SMEM)
PREPARED = (
    jax.ShapeDtypeStruct((SPLIT, TERMS, PLANE), BF16),
    jax.ShapeDtypeStruct((7 - SPLIT, TERMS, PLANE), BF16),
    jax.ShapeDtypeStruct((2, LANES, 2048), BF16),
    jax.ShapeDtypeStruct((344, UPPER_ROWS), BF16),
    jax.ShapeDtypeStruct((256, UPPER_ROWS), BF16),
    jax.ShapeDtypeStruct((2752, 216), BF16),
)


def make_first():
    return pl.pallas_call(
        first_kernel,
        out_shape=PREPARED[0],
        in_specs=[HBM_SPEC, HBM_SPEC],
        out_specs=HBM_SPEC,
        scratch_shapes=[
            pltpu.VMEM((TERMS, WIDTHS[0]), BF16),
            pltpu.VMEM((SPLIT, TERMS, PLANE), BF16),
            pltpu.SemaphoreType.DMA((2 * SPLIT,)),
        ],
        name="first",
    )


def make_second():
    return pl.pallas_call(
        second_kernel,
        out_shape=PREPARED[1:5],
        in_specs=[SMEM_SPEC, HBM_SPEC, VMEM_SPEC, HBM_SPEC],
        out_specs=(HBM_SPEC,) * 4,
        scratch_shapes=[
            pltpu.VMEM((TERMS, WIDTHS[1]), BF16),
            pltpu.VMEM((7 - SPLIT, TERMS, PLANE), BF16),
            pltpu.VMEM((2, LANES, 2048), BF16),
            pltpu.VMEM((344, UPPER_ROWS), BF16),
            pltpu.VMEM((256, UPPER_ROWS), BF16),
            pltpu.VMEM((LANES * 16, LANES), F32),
            pltpu.SemaphoreType.DMA((2 * (7 - SPLIT) + 3,)),
        ],
        name="second",
    )


def fill_window(window, left_ref, own_ref, right_ref, first_row):
    for bx in range(4):
        for by in range(4):
            for bz in range(4):
                if bx in (1, 2):
                    tile = own_ref[bx - 1, by, bz, first_row : first_row + 8, :]
                else:
                    at = 16 * (4 * by + bz) + first_row
                    tile = (left_ref if bx == 0 else right_ref)[at : at + 8, :]
                for i in range(2):
                    for j in range(2):
                        inner = i * 4 + j * 2
                        window[2 * bx + i, 2 * by + j, 2 * bz : 2 * bz + 2, :] = tile[inner : inner + 2, :]


def fill_slab(window, slab, tile, inner):
    for by in range(4):
        for bz in range(4):
            rows = tile(by, bz)
            for j in range(2):
                at = inner * 4 + j * 2
                window[slab, 2 * by + j, 2 * bz : 2 * bz + 2, :] = rows[at : at + 2, :]


def spread_slabs(window, rolled, spread, slabs):
    row8 = iota((8, LANES), 0)
    for x in range(slabs):
        for dz in range(3):
            for pair in range(3):
                first = pltpu.roll(window[x, 2 * pair + 1], 7 - dz, 0)
                second = pltpu.roll(window[x, 2 * pair + 2], (7 - dz + 4) % 8, 0)
                at = (x * 3 + dz) * 24 + 8 * pair
                rolled[at : at + 8, :] = jnp.where(row8 < 4, first, second)
    value = rolled[...]
    high = value.astype(BF16)
    rest = value - high.astype(F32)
    middle = rest.astype(BF16)
    low = (rest - middle.astype(F32)).astype(BF16)
    pieces = jnp.concatenate([high, middle, low], axis=1)
    column = iota((LANES, 2 * LANES), 1)
    row = iota((LANES, 2 * LANES), 0)
    for block in range(16):
        group, half = block // 2, block % 2
        wanted = (column // LANES + 2 * half) * SLOTS + 4 * group + column % LANES // SLOTS
        hot = (row == wanted).astype(F32).astype(BF16)
        found = jnp.dot(pieces, jnp.concatenate([hot, hot, hot], axis=0), preferred_element_type=F32)
        spread[2 * block] = found[:, 0:LANES]
        spread[2 * block + 1] = found[:, LANES : 2 * LANES]


def add_slab(mine, shift, spread, base, sums):
    tx = mine[0] - shift
    pot, fx, fy, fz = sums
    for ey in range(3):
        ty = mine[1] - float(ey - 1)
        for ez in range(3):
            tz = mine[2] - float(ez - 1)
            at = base + (ez * 24 + 4 * ey)
            for group in range(8):
                dx = tx - spread[4 * group, pl.ds(at, 16), :]
                dy = ty - spread[4 * group + 1, pl.ds(at, 16), :]
                dz = tz - spread[4 * group + 2, pl.ds(at, 16), :]
                inverse = lax.rsqrt(dx * dx + dy * dy + dz * dz + SOFTENING)
                weight = spread[4 * group + 3, pl.ds(at, 16), :] * inverse
                cubic = weight * (inverse * inverse)
                pot = pot + weight
                fx = fx + cubic * dx
                fy = fy + cubic * dy
                fz = fz + cubic * dz
    return pot, fx, fy, fz


def inner_kernel(own_ref, mine_ref, sum_ref, window, rolled, spread):
    for x in range(4):
        fill_slab(window, x, lambda by, bz: own_ref[x // 2, by, bz, 0:8, :], x % 2)
    spread_slabs(window, rolled, spread, 4)
    slot = iota((16, LANES), 1) % SLOTS
    for x in range(4):
        own = rolled[(x * 3 + 1) * 24 + 4 : (x * 3 + 1) * 24 + 20, :]
        for c in range(4):
            mine_ref[x, c] = jnp.take_along_axis(own, c * SLOTS + slot, axis=1)
    sum_ref[...] = jnp.zeros((4, 4, 16, LANES), F32)

    def one_pair(step, carry):
        target = (step + 1) // 3
        shift = (step + 1) - 3 * target - 1
        mine = [mine_ref[target, c] for c in range(3)]
        base = (target + shift) * 72
        sums = tuple(sum_ref[target, c] for c in range(4))
        sums = add_slab(mine, shift.astype(F32), spread, base, sums)
        for c in range(4):
            sum_ref[target, c] = sums[c]
        return carry

    lax.fori_loop(0, 10, one_pair, 0)


def make_inner():
    return pl.pallas_call(
        inner_kernel,
        out_shape=(
            jax.ShapeDtypeStruct((4, 4, 16, LANES), F32),
            jax.ShapeDtypeStruct((4, 4, 16, LANES), F32),
        ),
        scratch_shapes=[
            pltpu.VMEM((4, 8, 8, LANES), F32),
            pltpu.VMEM((288, LANES), F32),
            pltpu.VMEM((32, 288, LANES), F32),
        ],
        compiler_params=pltpu.CompilerParams(vmem_limit_bytes=56 << 20),
        name="inner",
    )


def outer_kernel(left_ref, right_ref, mine_ref, sum_ref, near_ref, window, rolled, spread):
    fill_slab(window, 0, lambda by, bz: left_ref[16 * (4 * by + bz) : 16 * (4 * by + bz) + 8, :], 1)
    fill_slab(window, 1, lambda by, bz: right_ref[16 * (4 * by + bz) : 16 * (4 * by + bz) + 8, :], 0)
    spread_slabs(window, rolled, spread, 2)
    part = iota((16, LANES), 1) // SLOTS
    keep = part == iota((16, LANES), 0) % 4
    itself = lax.rsqrt(jnp.full((16, LANES), SOFTENING, F32))

    def one_x(x, carry):
        sums = tuple(sum_ref[x, c] for c in range(4))
        mine = [mine_ref[x, c] for c in range(4)]

        def outside(sums):
            side = x // 3
            return add_slab(mine, (2 * side - 1).astype(F32), spread, side * 72, sums)

        sums = lax.cond((x == 0) | (x == 3), outside, lambda sums: sums, sums)
        totals = []
        for value in sums:
            value = value + pltpu.roll(value, 64, 1)
            value = value + pltpu.roll(value, 32, 1)
            totals.append(value)
        totals[0] = totals[0] - mine[3] * itself
        for c in range(4):
            chosen = jnp.where(keep, totals[c], 0.0)
            rows = [jnp.sum(chosen[4 * y : 4 * y + 4], axis=0, keepdims=True) for y in range(4)]
            near_ref[c, pl.ds(x, 1), :, :] = jnp.concatenate(rows, axis=0)[None]
        return carry

    lax.fori_loop(0, 4, one_x, 0)


def make_outer():
    return pl.pallas_call(
        outer_kernel,
        out_shape=jax.ShapeDtypeStruct((4, 4, 4, LANES), F32),
        scratch_shapes=[
            pltpu.VMEM((2, 8, 8, LANES), F32),
            pltpu.VMEM((144, LANES), F32),
            pltpu.VMEM((32, 144, LANES), F32),
        ],
        compiler_params=pltpu.CompilerParams(vmem_limit_bytes=24 << 20),
        name="outer",
    )


def far_kernel(
    index_ref,
    left_ref,
    own_ref,
    right_ref,
    middle_ref,
    upper_left_ref,
    upper_own_ref,
    upper_right_ref,
    pick_top_ref,
    shift_ref,
    local_ref,
    lattice_ref,
    gradient_ref,
    near_ref,
    wide_first_ref,
    wide_second_ref,
    value_ref,
    pick_upper_ref,
    pick_child_ref,
    pick_middle_ref,
    live_ref,
    potential_ref,
    field_ref,
    window,
    rolled,
    leaf_rows,
    small_rows,
    few,
    top,
    acc,
    local,
    shift_rows,
    local_rows,
):
    unpack_octants(shift_ref, shift_rows)
    unpack_octants(local_ref, local_rows)
    fill_window(window, left_ref, own_ref, right_ref, 8)
    row8 = iota((8, LANES), 0)
    row16 = iota((16, LANES), 0)
    rolled[:, 0:8, :] = jnp.zeros((7, 8, LANES), F32)
    rolled[:, 40:48, :] = jnp.zeros((7, 8, LANES), F32)

    def gather_plane(x, carry):
        for dz in range(-3, 4):
            for pair in range(4):
                even = pltpu.roll(window[x, 2 * pair], (16 - (dz + 2)) % 8, 0)
                odd = pltpu.roll(window[x, 2 * pair + 1], (16 - (dz + 2) + 4) % 8, 0)
                value = jnp.where(row8 < 4, even, odd)
                if dz == -3:
                    value = jnp.where(row8 % 2 == 1, value, 0.0)
                if dz == 3:
                    value = jnp.where(row8 % 2 == 0, value, 0.0)
                rolled[dz + 3, 8 + 8 * pair : 16 + 8 * pair, :] = value
        for dy in range(-3, 4):
            for dz in range(-3, 4):
                start = 8 + 4 * (dy + 2)
                value = rolled[dz + 3, start : start + 16, :]
                if dy == -3:
                    value = jnp.where(row16 // 4 % 2 == 1, value, 0.0)
                if dy == 3:
                    value = jnp.where(row16 // 4 % 2 == 0, value, 0.0)
                high, low = split(value)
                at = ((dy + 3) * 7 + dz + 3) * LANES
                leaf_rows[x, 0:16, at : at + LANES] = high
                leaf_rows[x, 16:32, at : at + LANES] = low
        return carry

    lax.fori_loop(0, 8, gather_plane, 0)

    def two(value):
        high, low = split(value)
        return jnp.concatenate([high, low], axis=1)

    uppers = two(
        jnp.concatenate(
            [
                upper_left_ref[...],
                upper_own_ref[...],
                upper_right_ref[...],
                jnp.zeros((UPPER_ROWS - 648, LANES), F32),
            ],
            axis=0,
        )
    )
    children = jnp.dot(pick_child_ref[...], uppers, preferred_element_type=F32)
    total = jnp.zeros((32, TERMS), F32)
    for octant in range(8):
        rows = children[32 * octant : 32 * octant + 32]
        both = jnp.concatenate([rows[:, :TERMS], rows[:, LANES : LANES + TERMS]], axis=0).astype(BF16)
        made = nt_dot(both, octant_operator(shift_rows, octant))
        total = total + made[:32] + made[32:]
    top[...] = jnp.zeros((32, LANES), F32)
    top[:, 0:TERMS] = total
    few[...] = jnp.zeros((2 * OFFSETS * 8 + 16, LANES), F32)
    from_upper = jnp.dot(pick_upper_ref[...], uppers, preferred_element_type=F32)
    from_top = jnp.dot(pick_top_ref[...], two(top[...]), preferred_element_type=F32)
    for side in range(2):
        span = slice(side * LANES, (side + 1) * LANES)
        few[pl.ds(2752 * side, 344, stride=8), :] = from_upper[:, span]
        few[pl.ds(2752 * side + 1, 344, stride=8), :] = from_top[:, span]
    middles = two(
        jnp.concatenate([left_ref[256:328, :], middle_ref[...], right_ref[256:328, :]], axis=0)
    )

    def small_plane(p, carry):
        rows = pick_middle_ref[pl.ds(pl.multiple_of(p * 392, 8), 392), :]
        found = jnp.dot(rows, middles, preferred_element_type=F32)
        for inside in range(49):
            base = pl.multiple_of(p * 392 + inside * 8, 8)
            for side in range(2):
                piece = found[8 * inside : 8 * inside + 8, side * LANES : (side + 1) * LANES]
                rest = few[pl.ds(base + 2752 * side, 8), :]
                small_rows[p, 16 * side : 16 * side + 16, inside * LANES : (inside + 1) * LANES] = (
                    jnp.concatenate([piece, rest], axis=0).astype(BF16)
                )
        return carry

    lax.fori_loop(0, 7, small_plane, 0)

    acc[...] = jnp.zeros((160, LANES), F32)
    for p in range(7):
        if p == 0:
            parts, places = [0, 2], [1, 3]
        elif p == 6:
            parts, places = [5, 7], [0, 2]
        else:
            parts, places = None, None
        if parts is None:
            left = leaf_rows[p - 1 : p + 3].reshape(128, PLANE)
        else:
            left = jnp.concatenate([leaf_rows[q] for q in parts], axis=0)
        left = jnp.concatenate([left, small_rows[p]], axis=0)
        found = nt_dot(left, wide_first_ref[p] if p < SPLIT else wide_second_ref[p - SPLIT])
        if parts is None:
            acc[:, 0:TERMS] += found
        else:
            for n, place in enumerate(places):
                acc[32 * place : 32 * place + 32, 0:TERMS] += found[32 * n : 32 * n + 32]
            acc[128:160, 0:TERMS] += found[64:96]

    far_middle = acc[128:136, :] + acc[144:152, :]
    far_rest = acc[136:144, :] + acc[152:160, :]
    root = jnp.sum(top[...], axis=0, keepdims=True)
    local[...] = jnp.zeros((8, LANES), F32)
    lattice = apply_op(jnp.broadcast_to(root, (8, LANES)), lattice_ref[...])
    local[:, 0:TERMS] = 0.125 * (far_rest[1:2, 0:TERMS] + lattice)
    own = index_ref[0] * 4 + index_ref[1] * 2 + index_ref[2]
    lowered = apply_op(local[...], octant_operator(local_rows, own))
    local[:, 0:TERMS] = 0.25 * far_rest[0:1, 0:TERMS] + lowered
    row_terms = iota((8, TERMS), 0)
    upper_local = local[...]
    spread = jnp.zeros((8, TERMS), F32)
    for octant in range(8):
        spread = spread + jnp.where(row_terms == octant, apply_op(upper_local, octant_operator(local_rows, octant)), 0.0)
    local[:, 0:TERMS] = 0.5 * far_middle[:, 0:TERMS] + spread
    middle_local = local[...]
    for x in range(4):
        base = 32 * x
        acc[base : base + 16, :] = acc[base : base + 16, :] + acc[base + 16 : base + 32, :]
    for octant in range(8):
        i, j, l = octant >> 2, octant >> 1 & 1, octant & 1
        made = apply_op(middle_local, octant_operator(local_rows, octant))
        for parent in range(8):
            bx, by, bz = parent >> 2, parent >> 1 & 1, parent & 1
            at = 32 * (2 * bx + i) + 4 * (2 * by + j) + 2 * bz + l
            acc[at : at + 1, 0:TERMS] += made[parent : parent + 1]
    for x in range(4):
        base = acc[32 * x : 32 * x + 16, :]
        high, low = split(base)
        both = jnp.concatenate([high, low], axis=0)
        listed = [base]
        for axis in range(3):
            made = jnp.dot(both, gradient_ref[axis], preferred_element_type=F32)
            listed.append(-(made[:16] + made[16:]))
        high, low = split(jnp.concatenate(listed, axis=0))
        first = value_ref[0, :, 512 * x : 512 * x + 512]
        second = value_ref[1, :, 512 * x : 512 * x + 512]
        found = jnp.dot(jnp.concatenate([high, low], axis=0), first, preferred_element_type=F32)
        found = found[:64] + found[64:] + jnp.dot(high, second, preferred_element_type=F32)
        keep = iota((4, LANES), 1) // SLOTS == iota((4, LANES), 0)
        for c in range(4):
            rows = []
            for y in range(4):
                piece = found[16 * c + 4 * y : 16 * c + 4 * y + 4, LANES * y : LANES * y + LANES]
                rows.append(jnp.sum(jnp.where(keep, piece, 0.0), axis=0, keepdims=True))
            value = (near_ref[c, x] + jnp.concatenate(rows, axis=0)) * live_ref[4 * x : 4 * x + 4, :]
            if c == 0:
                potential_ref[x] = value
            else:
                field_ref[c - 1, x] = value


def make_far():
    return pl.pallas_call(
        far_kernel,
        out_shape=(
            jax.ShapeDtypeStruct((4, 4, LANES), F32),
            jax.ShapeDtypeStruct((3, 4, 4, LANES), F32),
        ),
        in_specs=[SMEM_SPEC] + [VMEM_SPEC] * 20,
        scratch_shapes=[
            pltpu.VMEM((8, 8, 8, LANES), F32),
            pltpu.VMEM((7, 48, LANES), F32),
            pltpu.VMEM((8, 32, PLANE), BF16),
            pltpu.VMEM((7, 32, PLANE), BF16),
            pltpu.VMEM((2 * OFFSETS * 8 + 16, LANES), F32),
            pltpu.VMEM((32, LANES), F32),
            pltpu.VMEM((160, LANES), F32),
            pltpu.VMEM((8, LANES), F32),
            pltpu.VMEM((8 * TERMS, LANES), F32),
            pltpu.VMEM((8 * TERMS, LANES), F32),
        ],
        compiler_params=pltpu.CompilerParams(vmem_limit_bytes=24 << 20),
        name="far",
    )


def shifted(value, axis, shift):
    count = lax.axis_size(axis)
    return lax.ppermute(value, axis, [(i, (i + shift) % count) for i in range(count)])


def selections():
    slots = np.arange(344)
    dx = np.minimum(slots // 49, 6) - 3
    dy = slots // 7 % 7 - 3
    dz = slots % 7 - 3
    parent = np.arange(8)
    px, py, pz = parent >> 2, parent >> 1 & 1, parent & 1
    wide = [d[:, None] + p[None, :] + 2 for d, p in ((dx, px), (dy, py), (dz, pz))]
    fine = np.ones((344, 8), bool)
    for d, p in ((dx, px), (dy, py), (dz, pz)):
        fine &= (d[:, None] >= -2 - p[None, :]) & (d[:, None] <= 3 - p[None, :])
    column = ((wide[0] // 2 * 3 + wide[2] // 2) * 3 + wide[1] // 2) * 8
    column = column + wide[0] % 2 * 4 + wide[1] % 2 * 2 + wide[2] % 2
    middle = np.where(fine, column, -1).reshape(-1)
    top = ((dx % 4) * 2 + dy % 2) * 4 + dz % 4
    hot = [
        (place[:, None] == np.arange(width)[None, :]).astype(np.float32).astype(jnp.bfloat16)
        for place, width in ((middle, 216), (top, 32))
    ]
    return jnp.asarray(hot[0]), jnp.asarray(hot[1])


def per_device(positions, charges, counts, moment_shift, far_operators, local_shift, lattice_operator):
    index = jnp.stack([lax.axis_index(axis) % 2 for axis in ("gx", "gy", "gz")]).astype(jnp.int32)
    pos = positions.reshape(3, 16, LANES)
    shift = moment_shift.transpose(1, 0, 2)
    local = local_shift.transpose(1, 0, 2)
    comb, low, high, middle, alone, live = make_moments()(
        pos, charges.reshape(16, LANES), counts.reshape(16, 4), shift
    )
    pick_middle, pick_top = selections()

    def exchange(axis, low, high):
        return shifted(high, axis, 1), shifted(low, axis, -1)

    def pack(block, *rest):
        return jnp.concatenate([block.reshape(-1, LANES), *rest], axis=0)

    left, right = exchange("gy", low, high)
    near_copy = jnp.concatenate([comb.reshape(LANES, LANES), middle, alone], axis=0)
    near_copy, alone = lax.optimization_barrier((near_copy, alone))
    wide_first = make_first()(far_operators, near_copy)
    above = shifted(alone, "gy", -2)
    blocks = near_copy[:128].reshape(2, 2, 2, 16, LANES)
    middle, alone = near_copy[128:136], near_copy[136:144]
    sides = [left[:64].reshape(2, 1, 2, 16, LANES), right[:64].reshape(2, 1, 2, 16, LANES)]
    blocks = jnp.concatenate([sides[0], blocks, sides[1]], axis=1)
    middle = jnp.concatenate([left[64:72], middle, right[64:72]], axis=0)
    line = jnp.concatenate(
        [left[72:73], alone[0:1], right[72:73], above[0:1], jnp.zeros((4, LANES), F32)], axis=0
    )

    sends = (pack(blocks[:, :, 0], middle, line), pack(blocks[:, :, 1], middle, line))
    sends, blocks, middle, line, wide_first = lax.optimization_barrier(
        (sends, blocks, middle, line, wide_first)
    )
    left, right = exchange("gz", *sends)
    wide_second, values, pick_upper, pick_child = make_second()(index, far_operators, pos, wide_first)
    sides = [left[:128].reshape(2, 4, 1, 16, LANES), right[:128].reshape(2, 4, 1, 16, LANES)]
    blocks = jnp.concatenate([sides[0], blocks, sides[1]], axis=2)
    middle = jnp.concatenate([left[128:152], middle, right[128:152]], axis=0)
    line = jnp.concatenate([left[152:160], line, right[152:160]], axis=0)

    sends = (pack(blocks[0], middle, line), pack(blocks[1], middle, line))
    sends, blocks, middle, line, wide_second = lax.optimization_barrier(
        (sends, blocks, middle, line, wide_second)
    )
    left, right = exchange("gx", *sends)
    mine, sums = make_inner()(blocks)

    sheet = jnp.concatenate([left[328:352], line, right[328:352]], axis=0)
    sheet, sums = lax.optimization_barrier((sheet, sums))
    sheet = jnp.concatenate([shifted(sheet, "gz", 3), sheet, shifted(sheet, "gz", -3)], axis=0)
    upper_left = shifted(sheet, "gx", 3)
    upper_right = shifted(sheet, "gx", -3)

    near = make_outer()(left, right, mine, sums)
    gradients = jnp.asarray(gradient_tables(), BF16)
    return make_far()(
        index,
        left,
        blocks,
        right,
        middle,
        upper_left,
        sheet,
        upper_right,
        pick_top,
        shift,
        local,
        lattice_operator,
        gradients,
        near,
        wide_first,
        wide_second,
        values,
        pick_upper,
        pick_child,
        pick_middle,
        live,
    )


def solution(mesh):
    placed = (
        P(None, "gx", "gy", "gz"),
        P("gx", "gy", "gz"),
        P("gx", "gy", "gz"),
        P(),
        P(),
        P(),
        P(),
    )
    return jax.shard_map(
        per_device,
        mesh=mesh,
        in_specs=placed,
        out_specs=(P("gx", "gy", "gz"), P(None, "gx", "gy", "gz")),
        check_vma=False,
    )
```

```python
import jax
import jax.numpy as jnp
import numpy as np
from jax import lax
from jax.experimental import pallas as pl
from jax.experimental.pallas import tpu as pltpu
from jax.sharding import PartitionSpec as P

ORDER = 8
TERMS = 81
SLOTS = 32
SOFTENING = 0.0625
LANES = 128
OFFSETS = 343
PLANE = 49 * LANES
F32 = jnp.float32
BF16 = jnp.bfloat16


def exponent_table():
    listed = []
    for accumulated in range(ORDER + 1):
        for height in (0, 1):
            for power_x in range(accumulated - height + 1):
                listed.append((power_x, accumulated - height - power_x, height))
    return listed


EXPONENTS = exponent_table()


def offset_rows():
    rows, count = [], 0
    for x in range(-3, 4):
        for y in range(-3, 4):
            for z in range(-3, 4):
                if max(abs(x), abs(y), abs(z)) >= 2:
                    rows.append(count)
                    count += 1
                else:
                    rows.append(-1)
    return rows


OFFSET_ROWS = offset_rows()


def gradient_tables():
    place = {e: k for k, e in enumerate(EXPONENTS)}
    tables = np.zeros((3, LANES, LANES), np.float32)
    for k, e in enumerate(EXPONENTS):
        for axis in range(3):
            if e[axis] > 0:
                lowered = list(e)
                lowered[axis] -= 1
                tables[axis, k, place[tuple(lowered)]] = e[axis]
    return tables


def full_spec(shape):
    return pl.BlockSpec(shape, lambda *_: (0,) * len(shape))


def nt_dot(left, right):
    return lax.dot_general(left, right, (((1,), (1,)), ((), ())), preferred_element_type=F32)


def split(value):
    upper = value.astype(BF16)
    lower = (value - upper.astype(F32)).astype(BF16)
    return upper, lower


def stack_split(value):
    upper = value.astype(BF16).astype(F32)
    return jnp.concatenate([upper, value - upper], axis=0).astype(BF16)


def apply_op(value, operator):
    both = nt_dot(stack_split(value)[:, :TERMS], operator)
    return both[:8] + both[8:]


def unpack_octants(source_ref, rows):
    rows[:, 0:TERMS] = source_ref[...].astype(F32).reshape(8 * TERMS, TERMS)


def octant_operator(rows, octant):
    return rows[pl.ds(octant, TERMS, stride=8), :][:, :TERMS].astype(BF16)


def iota(shape, axis):
    return lax.broadcasted_iota(jnp.int32, shape, axis)


def powers(value):
    listed = [None, value]
    for _ in range(2, ORDER + 1):
        listed.append(listed[-1] * value)
    return listed


def write_monomials(target, positions, factor):
    px = powers(positions[0] - 0.5)
    py = powers(positions[1] - 0.5)
    pz = positions[2] - 0.5
    for k, (a, b, c) in enumerate(EXPONENTS):
        value = factor
        if a:
            value = px[a] if value is None else value * px[a]
        if b:
            value = py[b] if value is None else value * py[b]
        if c:
            value = pz if value is None else value * pz
        if value is None:
            value = jnp.ones_like(pz)
        target[k * 16 : (k + 1) * 16, :] = value
    target[TERMS * 16 : LANES * 16, :] = jnp.zeros(((LANES - TERMS) * 16, LANES), F32)


def moments_kernel(
    pos_hbm,
    charge_hbm,
    count_hbm,
    shift_hbm,
    comb_ref,
    low_ref,
    high_ref,
    upper_ref,
    alone_ref,
    live_ref,
    pos_ref,
    charge_ref,
    count_ref,
    shift_ref,
    mono,
    leaf,
    rows,
    sems,
):
    loads = [
        pltpu.make_async_copy(a, b, sems.at[n])
        for n, (a, b) in enumerate(
            (
                (count_hbm, count_ref),
                (charge_hbm, charge_ref),
                (pos_hbm, pos_ref),
                (shift_hbm, shift_ref),
            )
        )
    ]
    for load in loads:
        load.start()
    for load in loads[:3]:
        load.wait()
    lane = iota((16, LANES), 1)
    count = jnp.zeros((16, LANES), jnp.int32)
    for z in range(4):
        count = jnp.where(lane // SLOTS == z, count_ref[:, z : z + 1], count)
    live = (lane % SLOTS < count).astype(F32)
    live_ref[...] = live
    weight = charge_ref[...] * live
    write_monomials(mono, (pos_ref[0], pos_ref[1], pos_ref[2]), weight)
    uppers, lowers = [], []
    for row in range(16):
        high, low = split(mono[pl.ds(row, LANES, stride=16), :])
        uppers.append(high)
        lowers.append(low)
    row = iota((64, 2048), 0)
    x = (row >> 5 & 1) * 2 + (row >> 2 & 1)
    y = (row >> 4 & 1) * 2 + (row >> 1 & 1)
    z = (row >> 3 & 1) * 2 + (row & 1)
    picker = (iota((64, 2048), 1) // SLOTS == (x * 4 + y) * 4 + z).astype(F32).astype(BF16)
    moments = nt_dot(picker, jnp.concatenate(uppers, axis=1)) + nt_dot(
        picker, jnp.concatenate(lowers, axis=1)
    )
    leaf[...] = moments
    comb_ref[:, 8:16, :] = moments.reshape(8, 8, LANES)
    lane8 = iota((8, LANES), 1)
    index = (iota((8, LANES), 0) % 4) * SLOTS + lane8 % SLOTS
    for xy in range(16):
        pieces = [pos_ref[c, xy : xy + 1, :] for c in range(3)] + [weight[xy : xy + 1, :]]
        merged = None
        for c, piece in enumerate(pieces):
            moved = jnp.take_along_axis(jnp.broadcast_to(piece, (8, LANES)), index, axis=1)
            merged = moved if merged is None else jnp.where(lane8 // SLOTS == c, moved, merged)
        cx, cy = xy // 4, xy % 4
        for half in range(2):
            parent = (cx // 2) * 4 + (cy // 2) * 2 + half
            inner = (cx % 2) * 4 + (cy % 2) * 2
            comb_ref[parent, inner : inner + 2, :] = merged[2 * half : 2 * half + 2, :]
    loads[3].wait()
    unpack_octants(shift_ref, rows)
    operators = [octant_operator(rows, octant) for octant in range(8)]
    upper_ref[...] = jnp.zeros((8, LANES), F32)
    middle = jnp.zeros((8, TERMS), F32)
    for octant in range(8):
        middle = middle + apply_op(leaf[pl.ds(octant, 8, stride=8), :], operators[octant])
    upper_ref[0:8, 0:TERMS] = middle
    wide = upper_ref[...]
    total = jnp.zeros((8, TERMS), F32)
    row8 = iota((8, TERMS), 0)
    for octant in range(8):
        total = total + jnp.where(row8 == octant, apply_op(wide, operators[octant]), 0.0)
    alone_ref[...] = jnp.zeros((8, LANES), F32)
    alone_ref[0:1, 0:TERMS] = jnp.sum(total, axis=0, keepdims=True)
    for half, target in enumerate((low_ref, high_ref)):
        for bx in range(2):
            for bz in range(2):
                at = 16 * (2 * bx + bz)
                target[at : at + 16, :] = comb_ref[4 * bx + 2 * half + bz]
        target[64:72, :] = upper_ref[...]
        target[72:80, :] = alone_ref[...]


def make_moments():
    return pl.pallas_call(
        moments_kernel,
        out_shape=(
            jax.ShapeDtypeStruct((8, 16, LANES), F32),
            jax.ShapeDtypeStruct((80, LANES), F32),
            jax.ShapeDtypeStruct((80, LANES), F32),
            jax.ShapeDtypeStruct((8, LANES), F32),
            jax.ShapeDtypeStruct((8, LANES), F32),
            jax.ShapeDtypeStruct((16, LANES), F32),
        ),
        in_specs=[pl.BlockSpec(memory_space=pl.ANY)] * 4,
        scratch_shapes=[
            pltpu.VMEM((3, 16, LANES), F32),
            pltpu.VMEM((16, LANES), F32),
            pltpu.VMEM((16, 4), jnp.int32),
            pltpu.VMEM((TERMS, 8, TERMS), BF16),
            pltpu.VMEM((LANES * 16, LANES), F32),
            pltpu.VMEM((64, LANES), F32),
            pltpu.VMEM((8 * TERMS, LANES), F32),
            pltpu.SemaphoreType.DMA((4,)),
        ],
        name="moments",
    )


UPPER_ROWS = 768
CUTS = [-(-row * TERMS // LANES) * LANES for row in (0, 49, 98, 138, 178, 218, 267)] + [25600]


def spot(relative_x, relative_z, relative_y):
    x = (relative_x + 3 & 7) + 1
    z = (relative_z + 3 & 7) + 1
    xb = x * 11 >> 5
    zb = z * 11 >> 5
    return xb * 216 + zb * 72 + (x - 3 * xb) * 24 + (z - 3 * zb) * 8 + (relative_y + 1 & 3)


def write_hot(target, column):
    rows = column.shape[0]
    lane = iota((rows, LANES), 1)
    for block in range(UPPER_ROWS // LANES):
        hot = (lane + block * LANES == column).astype(F32).astype(BF16)
        target[:, block * LANES : (block + 1) * LANES] = hot


def widen(far_hbm, wide_hbm, far_ref, wide_ref, sems, first, last):
    start = max(CUTS[first] - LANES, 0)
    edges = [start] + CUTS[first + 1 : last + 1]
    count = last - first
    loads = []
    for p in range(count):
        size = edges[p + 1] - edges[p]
        loads.append(
            pltpu.make_async_copy(
                far_hbm.at[:, pl.ds(edges[p], size)], far_ref.at[:, pl.ds(edges[p] - start, size)], sems.at[p]
            )
        )
    stores = [pltpu.make_async_copy(wide_ref.at[p], wide_hbm.at[p], sems.at[count + p]) for p in range(count)]
    for load in loads:
        load.start()

    def finish():
        lane = iota((TERMS, LANES), 1)
        for slot in range(49 * first, 49 * last):
            source = OFFSET_ROWS[slot]
            plane, inside = slot // 49 - first, slot % 49
            if inside == 0:
                loads[plane].wait()
            span = slice(inside * LANES, (inside + 1) * LANES)
            if source < 0:
                wide_ref[plane, :, span] = jnp.zeros((TERMS, LANES), BF16)
            else:
                base, shift = divmod(source * TERMS - start, LANES)
                merged = far_ref[:, base * LANES : (base + 1) * LANES]
                if shift + TERMS > LANES:
                    following = far_ref[:, (base + 1) * LANES : (base + 2) * LANES]
                    merged = jnp.where(lane >= shift, merged.astype(F32), following.astype(F32))
                    merged = merged.astype(BF16)
                if shift:
                    merged = pltpu.roll(merged, LANES - shift, 1)
                wide_ref[plane, :, span] = merged
            if inside == 48:
                stores[plane].start()
        for store in stores:
            store.wait()

    return finish


SPLIT = 4
WIDTHS = (CUTS[SPLIT], 25600 - CUTS[SPLIT] + LANES)


def first_kernel(far_hbm, after_ref, wide_hbm, far_ref, wide_ref, sems):
    widen(far_hbm, wide_hbm, far_ref, wide_ref, sems, 0, SPLIT)()


def second_kernel(
    index_ref,
    far_hbm,
    pos_ref,
    after_ref,
    wide_hbm,
    value_hbm,
    upper_hbm,
    child_hbm,
    far_ref,
    wide_ref,
    value_ref,
    upper_ref,
    child_ref,
    mono,
    sems,
):
    finish = widen(far_hbm, wide_hbm, far_ref, wide_ref, sems, SPLIT, 7)
    parity_x, parity_y, parity_z = index_ref[0], index_ref[1], index_ref[2]
    row = iota((256, LANES), 0)
    octant, box = row >> 5, row & 31
    vx = 2 * (box >> 3) + (octant >> 2) - parity_x
    vy = 2 * (box >> 2 & 1) + (octant >> 1 & 1) - parity_y
    vz = 2 * (box & 3) + (octant & 1) - parity_z
    write_hot(child_ref, spot(vx, vz, vy))
    row = iota((344, LANES), 0)
    plane = row * 1338 >> 16
    inside = row - plane * 49
    line = inside * 37 >> 8
    dx, dy, dz = plane - 3, line - 3, inside - line * 7 - 3
    fine = (dx >= -2 - parity_x) & (dx <= 3 - parity_x)
    fine = fine & (dy >= -2 - parity_y) & (dy <= 3 - parity_y)
    fine = fine & (dz >= -2 - parity_z) & (dz <= 3 - parity_z)
    write_hot(upper_ref, jnp.where(fine, spot(dx, dz, dy), -1))
    write_monomials(mono, (pos_ref[0], pos_ref[1], pos_ref[2]), None)
    for row in range(16):
        high, low = split(mono[pl.ds(row, LANES, stride=16), :])
        value_ref[0, :, row * LANES : (row + 1) * LANES] = high
        value_ref[1, :, row * LANES : (row + 1) * LANES] = low
    outs = [
        pltpu.make_async_copy(a, b, sems.at[2 * (7 - SPLIT) + n])
        for n, (a, b) in enumerate(((value_ref, value_hbm), (upper_ref, upper_hbm), (child_ref, child_hbm)))
    ]
    for out in outs:
        out.start()
    finish()
    for out in outs:
        out.wait()


VMEM_SPEC = pl.BlockSpec(memory_space=pltpu.VMEM)
HBM_SPEC = pl.BlockSpec(memory_space=pl.ANY)
SMEM_SPEC = pl.BlockSpec(memory_space=pltpu.SMEM)
PREPARED = (
    jax.ShapeDtypeStruct((SPLIT, TERMS, PLANE), BF16),
    jax.ShapeDtypeStruct((7 - SPLIT, TERMS, PLANE), BF16),
    jax.ShapeDtypeStruct((2, LANES, 2048), BF16),
    jax.ShapeDtypeStruct((344, UPPER_ROWS), BF16),
    jax.ShapeDtypeStruct((256, UPPER_ROWS), BF16),
    jax.ShapeDtypeStruct((2752, 216), BF16),
)


def make_first():
    return pl.pallas_call(
        first_kernel,
        out_shape=PREPARED[0],
        in_specs=[HBM_SPEC, HBM_SPEC],
        out_specs=HBM_SPEC,
        scratch_shapes=[
            pltpu.VMEM((TERMS, WIDTHS[0]), BF16),
            pltpu.VMEM((SPLIT, TERMS, PLANE), BF16),
            pltpu.SemaphoreType.DMA((2 * SPLIT,)),
        ],
        name="first",
    )


def make_second():
    return pl.pallas_call(
        second_kernel,
        out_shape=PREPARED[1:5],
        in_specs=[SMEM_SPEC, HBM_SPEC, VMEM_SPEC, HBM_SPEC],
        out_specs=(HBM_SPEC,) * 4,
        scratch_shapes=[
            pltpu.VMEM((TERMS, WIDTHS[1]), BF16),
            pltpu.VMEM((7 - SPLIT, TERMS, PLANE), BF16),
            pltpu.VMEM((2, LANES, 2048), BF16),
            pltpu.VMEM((344, UPPER_ROWS), BF16),
            pltpu.VMEM((256, UPPER_ROWS), BF16),
            pltpu.VMEM((LANES * 16, LANES), F32),
            pltpu.SemaphoreType.DMA((2 * (7 - SPLIT) + 3,)),
        ],
        name="second",
    )


def fill_window(window, left_ref, own_ref, right_ref, first_row):
    for bx in range(4):
        for by in range(4):
            for bz in range(4):
                if bx in (1, 2):
                    tile = own_ref[bx - 1, by, bz, first_row : first_row + 8, :]
                else:
                    at = 16 * (4 * by + bz) + first_row
                    tile = (left_ref if bx == 0 else right_ref)[at : at + 8, :]
                for i in range(2):
                    for j in range(2):
                        inner = i * 4 + j * 2
                        window[2 * bx + i, 2 * by + j, 2 * bz : 2 * bz + 2, :] = tile[inner : inner + 2, :]


def fill_slab(window, slab, tile, inner):
    for by in range(4):
        for bz in range(4):
            rows = tile(by, bz)
            for j in range(2):
                at = inner * 4 + j * 2
                window[slab, 2 * by + j, 2 * bz : 2 * bz + 2, :] = rows[at : at + 2, :]


def spread_slabs(window, rolled, spread, slabs, used):
    row8 = iota((8, LANES), 0)
    for x in range(slabs):
        for dz in range(3):
            for pair in range(3):
                first = pltpu.roll(window[x, 2 * pair + 1], 7 - dz, 0)
                second = pltpu.roll(window[x, 2 * pair + 2], (7 - dz + 4) % 8, 0)
                at = (x * 3 + dz) * 24 + 8 * pair
                rolled[at : at + 8, :] = jnp.where(row8 < 4, first, second)
    value = rolled[0 : used * 72, :]
    high = value.astype(BF16)
    rest = value - high.astype(F32)
    middle = rest.astype(BF16)
    low = (rest - middle.astype(F32)).astype(BF16)
    pieces = jnp.concatenate([high, middle, low], axis=1)
    column = iota((LANES, 2 * LANES), 1)
    row = iota((LANES, 2 * LANES), 0)
    for block in range(16):
        group, half = block // 2, block % 2
        wanted = (column // LANES + 2 * half) * SLOTS + 4 * group + column % LANES // SLOTS
        hot = (row == wanted).astype(F32).astype(BF16)
        found = jnp.dot(pieces, jnp.concatenate([hot, hot, hot], axis=0), preferred_element_type=F32)
        spread[2 * block] = found[:, 0:LANES]
        spread[2 * block + 1] = found[:, LANES : 2 * LANES]


def add_slab(mine, shift, spread, base, sums):
    tx = mine[0] - shift
    pot, fx, fy, fz = sums
    for ey in range(3):
        ty = mine[1] - float(ey - 1)
        for ez in range(3):
            tz = mine[2] - float(ez - 1)
            at = base + (ez * 24 + 4 * ey)
            for group in range(8):
                dx = tx - spread[4 * group, pl.ds(at, 16), :]
                dy = ty - spread[4 * group + 1, pl.ds(at, 16), :]
                dz = tz - spread[4 * group + 2, pl.ds(at, 16), :]
                inverse = lax.rsqrt(dx * dx + dy * dy + dz * dz + SOFTENING)
                weight = spread[4 * group + 3, pl.ds(at, 16), :] * inverse
                cubic = weight * (inverse * inverse)
                pot = pot + weight
                fx = fx + cubic * dx
                fy = fy + cubic * dy
                fz = fz + cubic * dz
    return pot, fx, fy, fz


def inner_kernel(own_ref, mine_ref, sum_ref, window, rolled, spread):
    for x in range(4):
        fill_slab(window, x, lambda by, bz: own_ref[x // 2, by, bz, 0:8, :], x % 2)
    spread_slabs(window, rolled, spread, 4, 3)
    slot = iota((16, LANES), 1) % SLOTS
    for x in range(4):
        own = rolled[(x * 3 + 1) * 24 + 4 : (x * 3 + 1) * 24 + 20, :]
        for c in range(4):
            mine_ref[x, c] = jnp.take_along_axis(own, c * SLOTS + slot, axis=1)
    sum_ref[...] = jnp.zeros((4, 4, 16, LANES), F32)

    def one_pair(step, carry):
        source = (step + 1) // 3
        shift = 1 - ((step + 1) - 3 * source)
        target = source - shift
        mine = [mine_ref[target, c] for c in range(3)]
        base = source * 72
        sums = tuple(sum_ref[target, c] for c in range(4))
        sums = add_slab(mine, shift.astype(F32), spread, base, sums)
        for c in range(4):
            sum_ref[target, c] = sums[c]
        return carry

    lax.fori_loop(0, 8, one_pair, 0)


def make_inner():
    return pl.pallas_call(
        inner_kernel,
        out_shape=(
            jax.ShapeDtypeStruct((4, 4, 16, LANES), F32),
            jax.ShapeDtypeStruct((4, 4, 16, LANES), F32),
        ),
        scratch_shapes=[
            pltpu.VMEM((4, 8, 8, LANES), F32),
            pltpu.VMEM((288, LANES), F32),
            pltpu.VMEM((32, 216, LANES), F32),
        ],
        compiler_params=pltpu.CompilerParams(vmem_limit_bytes=40 << 20),
        name="inner",
    )


def outer_kernel(left_ref, own_ref, right_ref, mine_ref, sum_ref, near_ref, sums_ref, window, rolled, spread):
    fill_slab(window, 0, lambda by, bz: left_ref[16 * (4 * by + bz) : 16 * (4 * by + bz) + 8, :], 1)
    fill_slab(window, 1, lambda by, bz: right_ref[16 * (4 * by + bz) : 16 * (4 * by + bz) + 8, :], 0)
    fill_slab(window, 2, lambda by, bz: own_ref[1, by, bz, 0:8, :], 1)
    spread_slabs(window, rolled, spread, 3, 3)
    sums_ref[...] = sum_ref[...]

    def one_pair(step, carry):
        target = jnp.where(step == 0, 0, jnp.where(step == 1, 2, 3))
        slab = jnp.where(step == 0, 0, jnp.where(step == 3, 1, 2))
        shift = jnp.where(step == 0, -1, jnp.where(step == 2, 0, 1))
        mine = [mine_ref[target, c] for c in range(3)]
        sums = tuple(sums_ref[target, c] for c in range(4))
        sums = add_slab(mine, shift.astype(F32), spread, slab * 72, sums)
        for c in range(4):
            sums_ref[target, c] = sums[c]
        return carry

    lax.fori_loop(0, 4, one_pair, 0)
    part = iota((16, LANES), 1) // SLOTS
    keep = part == iota((16, LANES), 0) % 4
    itself = lax.rsqrt(jnp.full((16, LANES), SOFTENING, F32))

    for x in range(4):
        totals = []
        for c in range(4):
            value = sums_ref[x, c]
            value = value + pltpu.roll(value, 64, 1)
            value = value + pltpu.roll(value, 32, 1)
            totals.append(value)
        totals[0] = totals[0] - mine_ref[x, 3] * itself
        for c in range(4):
            chosen = jnp.where(keep, totals[c], 0.0)
            rows = [jnp.sum(chosen[4 * y : 4 * y + 4], axis=0, keepdims=True) for y in range(4)]
            near_ref[c, x] = jnp.concatenate(rows, axis=0)


def make_outer():
    return pl.pallas_call(
        outer_kernel,
        out_shape=jax.ShapeDtypeStruct((4, 4, 4, LANES), F32),
        scratch_shapes=[
            pltpu.VMEM((4, 4, 16, LANES), F32),
            pltpu.VMEM((3, 8, 8, LANES), F32),
            pltpu.VMEM((216, LANES), F32),
            pltpu.VMEM((32, 216, LANES), F32),
        ],
        compiler_params=pltpu.CompilerParams(vmem_limit_bytes=40 << 20),
        name="outer",
    )


def two(value):
    return jnp.concatenate(split(value), axis=1)


def fetch_kernel(
    first_hbm,
    second_hbm,
    pick_middle_ref,
    left_ref,
    own_ref,
    right_ref,
    middle_ref,
    after_ref,
    wide_first_ref,
    wide_second_ref,
    middle_rows,
    leaf_rows,
    window,
    rolled,
    sems,
):
    copies = [
        pltpu.make_async_copy(first_hbm, wide_first_ref, sems.at[0]),
        pltpu.make_async_copy(second_hbm, wide_second_ref, sems.at[1]),
    ]
    for copy in copies:
        copy.start()
    fill_window(window, left_ref, own_ref, right_ref, 8)
    row8 = iota((8, LANES), 0)
    row16 = iota((16, LANES), 0)
    rolled[:, 0:8, :] = jnp.zeros((7, 8, LANES), F32)
    rolled[:, 40:48, :] = jnp.zeros((7, 8, LANES), F32)

    def gather_plane(x, carry):
        for dz in range(-3, 4):
            for pair in range(4):
                even = pltpu.roll(window[x, 2 * pair], (16 - (dz + 2)) % 8, 0)
                odd = pltpu.roll(window[x, 2 * pair + 1], (16 - (dz + 2) + 4) % 8, 0)
                value = jnp.where(row8 < 4, even, odd)
                if dz == -3:
                    value = jnp.where(row8 % 2 == 1, value, 0.0)
                if dz == 3:
                    value = jnp.where(row8 % 2 == 0, value, 0.0)
                rolled[dz + 3, 8 + 8 * pair : 16 + 8 * pair, :] = value
        for dy in range(-3, 4):
            for dz in range(-3, 4):
                start = 8 + 4 * (dy + 2)
                value = rolled[dz + 3, start : start + 16, :]
                if dy == -3:
                    value = jnp.where(row16 // 4 % 2 == 1, value, 0.0)
                if dy == 3:
                    value = jnp.where(row16 // 4 % 2 == 0, value, 0.0)
                high, low = split(value)
                at = ((dy + 3) * 7 + dz + 3) * LANES
                leaf_rows[x, 0:16, at : at + LANES] = high
                leaf_rows[x, 16:32, at : at + LANES] = low
        return carry

    lax.fori_loop(0, 8, gather_plane, 0)
    middles = two(
        jnp.concatenate([left_ref[256:328, :], middle_ref[...], right_ref[256:328, :]], axis=0)
    )

    def middle_plane(p, carry):
        rows = pick_middle_ref[pl.ds(pl.multiple_of(p * 392, 8), 392), :]
        found = jnp.dot(rows, middles, preferred_element_type=F32)
        for inside in range(49):
            piece = found[8 * inside : 8 * inside + 8]
            middle_rows[p, :, inside * LANES : (inside + 1) * LANES] = jnp.concatenate(
                [piece[:, 0:LANES], piece[:, LANES : 2 * LANES]], axis=0
            ).astype(BF16)
        return carry

    lax.fori_loop(0, 7, middle_plane, 0)
    for copy in copies:
        copy.wait()


FETCHED = (
    PREPARED[0],
    PREPARED[1],
    jax.ShapeDtypeStruct((7, 16, PLANE), BF16),
    jax.ShapeDtypeStruct((8, 32, PLANE), BF16),
)


def make_fetch():
    return pl.pallas_call(
        fetch_kernel,
        out_shape=FETCHED,
        in_specs=[HBM_SPEC] * 2 + [VMEM_SPEC] * 5 + [HBM_SPEC],
        out_specs=(VMEM_SPEC,) * len(FETCHED),
        scratch_shapes=[
            pltpu.VMEM((8, 8, 8, LANES), F32),
            pltpu.VMEM((7, 48, LANES), F32),
            pltpu.SemaphoreType.DMA((2,)),
        ],
        compiler_params=pltpu.CompilerParams(vmem_limit_bytes=FETCH_LIMIT << 20),
        name="fetch",
    )


FETCH_LIMIT = 36


def far_kernel(
    index_ref,
    upper_left_ref,
    upper_own_ref,
    upper_right_ref,
    pick_top_ref,
    shift_ref,
    local_ref,
    lattice_ref,
    gradient_ref,
    near_ref,
    wide_first_ref,
    wide_second_ref,
    value_ref,
    pick_upper_ref,
    pick_child_ref,
    middle_rows,
    leaf_rows,
    live_ref,
    potential_ref,
    field_ref,
    few_rows,
    few,
    top,
    acc,
    local,
    shift_rows,
    local_rows,
):
    unpack_octants(shift_ref, shift_rows)
    unpack_octants(local_ref, local_rows)
    uppers = two(
        jnp.concatenate(
            [
                upper_left_ref[...],
                upper_own_ref[...],
                upper_right_ref[...],
                jnp.zeros((UPPER_ROWS - 648, LANES), F32),
            ],
            axis=0,
        )
    )
    children = jnp.dot(pick_child_ref[...], uppers, preferred_element_type=F32)
    total = jnp.zeros((32, TERMS), F32)
    for octant in range(8):
        rows = children[32 * octant : 32 * octant + 32]
        both = jnp.concatenate([rows[:, :TERMS], rows[:, LANES : LANES + TERMS]], axis=0).astype(BF16)
        made = nt_dot(both, octant_operator(shift_rows, octant))
        total = total + made[:32] + made[32:]
    top[...] = jnp.zeros((32, LANES), F32)
    top[:, 0:TERMS] = total
    few[...] = jnp.zeros((OFFSETS * 8 + 8, LANES), F32)
    from_upper = jnp.dot(pick_upper_ref[...], uppers, preferred_element_type=F32)
    from_top = jnp.dot(pick_top_ref[...], two(top[...]), preferred_element_type=F32)
    for side in range(2):
        span = slice(side * LANES, (side + 1) * LANES)
        few[pl.ds(2 * side, 344, stride=8), :] = from_upper[:, span]
        few[pl.ds(2 * side + 1, 344, stride=8), :] = from_top[:, span]
    none = jnp.zeros((8, LANES), F32)

    def few_plane(p, carry):
        for inside in range(49):
            rows = few[pl.ds(pl.multiple_of(p * 392 + inside * 8, 8), 8), :]
            few_rows[p, :, inside * LANES : (inside + 1) * LANES] = jnp.concatenate(
                [rows, none], axis=0
            ).astype(BF16)
        return carry

    lax.fori_loop(0, 7, few_plane, 0)

    acc[...] = jnp.zeros((160, LANES), F32)
    for p in range(7):
        if p == 0:
            parts, places = [0, 2], [1, 3]
        elif p == 6:
            parts, places = [5, 7], [0, 2]
        else:
            parts, places = None, None
        if parts is None:
            left = leaf_rows[p - 1 : p + 3].reshape(128, PLANE)
        else:
            left = jnp.concatenate([leaf_rows[q] for q in parts], axis=0)
        left = jnp.concatenate([left, middle_rows[p], few_rows[p]], axis=0)
        found = nt_dot(left, wide_first_ref[p] if p < SPLIT else wide_second_ref[p - SPLIT])
        if parts is None:
            acc[:, 0:TERMS] += found
        else:
            for n, place in enumerate(places):
                acc[32 * place : 32 * place + 32, 0:TERMS] += found[32 * n : 32 * n + 32]
            acc[128:160, 0:TERMS] += found[64:96]

    far_middle = acc[128:136, :] + acc[136:144, :]
    far_rest = acc[144:146, :] + acc[146:148, :]
    root = jnp.sum(top[...], axis=0, keepdims=True)
    local[...] = jnp.zeros((8, LANES), F32)
    lattice = apply_op(jnp.broadcast_to(root, (8, LANES)), lattice_ref[...])
    local[:, 0:TERMS] = 0.125 * (far_rest[1:2, 0:TERMS] + lattice)
    own = index_ref[0] * 4 + index_ref[1] * 2 + index_ref[2]
    lowered = apply_op(local[...], octant_operator(local_rows, own))
    local[:, 0:TERMS] = 0.25 * far_rest[0:1, 0:TERMS] + lowered
    row_terms = iota((8, TERMS), 0)
    upper_local = local[...]
    spread = jnp.zeros((8, TERMS), F32)
    for octant in range(8):
        spread = spread + jnp.where(row_terms == octant, apply_op(upper_local, octant_operator(local_rows, octant)), 0.0)
    local[:, 0:TERMS] = 0.5 * far_middle[:, 0:TERMS] + spread
    middle_local = local[...]
    for x in range(4):
        base = 32 * x
        acc[base : base + 16, :] = acc[base : base + 16, :] + acc[base + 16 : base + 32, :]
    for octant in range(8):
        i, j, l = octant >> 2, octant >> 1 & 1, octant & 1
        made = apply_op(middle_local, octant_operator(local_rows, octant))
        for parent in range(8):
            bx, by, bz = parent >> 2, parent >> 1 & 1, parent & 1
            at = 32 * (2 * bx + i) + 4 * (2 * by + j) + 2 * bz + l
            acc[at : at + 1, 0:TERMS] += made[parent : parent + 1]
    for x in range(4):
        base = acc[32 * x : 32 * x + 16, :]
        high, low = split(base)
        both = jnp.concatenate([high, low], axis=0)
        listed = [base]
        for axis in range(3):
            made = jnp.dot(both, gradient_ref[axis], preferred_element_type=F32)
            listed.append(-(made[:16] + made[16:]))
        high, low = split(jnp.concatenate(listed, axis=0))
        first = value_ref[0, :, 512 * x : 512 * x + 512]
        second = value_ref[1, :, 512 * x : 512 * x + 512]
        found = jnp.dot(jnp.concatenate([high, low], axis=0), first, preferred_element_type=F32)
        found = found[:64] + found[64:] + jnp.dot(high, second, preferred_element_type=F32)
        keep = iota((4, LANES), 1) // SLOTS == iota((4, LANES), 0)
        for c in range(4):
            rows = []
            for y in range(4):
                piece = found[16 * c + 4 * y : 16 * c + 4 * y + 4, LANES * y : LANES * y + LANES]
                rows.append(jnp.sum(jnp.where(keep, piece, 0.0), axis=0, keepdims=True))
            value = (near_ref[c, x] + jnp.concatenate(rows, axis=0)) * live_ref[4 * x : 4 * x + 4, :]
            if c == 0:
                potential_ref[x] = value
            else:
                field_ref[c - 1, x] = value


def make_far():
    return pl.pallas_call(
        far_kernel,
        out_shape=(
            jax.ShapeDtypeStruct((4, 4, LANES), F32),
            jax.ShapeDtypeStruct((3, 4, 4, LANES), F32),
        ),
        in_specs=[SMEM_SPEC] + [VMEM_SPEC] * 17,
        scratch_shapes=[
            pltpu.VMEM((7, 16, PLANE), BF16),
            pltpu.VMEM((OFFSETS * 8 + 8, LANES), F32),
            pltpu.VMEM((32, LANES), F32),
            pltpu.VMEM((160, LANES), F32),
            pltpu.VMEM((8, LANES), F32),
            pltpu.VMEM((8 * TERMS, LANES), F32),
            pltpu.VMEM((8 * TERMS, LANES), F32),
        ],
        compiler_params=pltpu.CompilerParams(vmem_limit_bytes=24 << 20),
        name="far",
    )


def shifted(value, axis, shift):
    count = lax.axis_size(axis)
    return lax.ppermute(value, axis, [(i, (i + shift) % count) for i in range(count)])


def selections():
    slots = np.arange(344)
    dx = np.minimum(slots // 49, 6) - 3
    dy = slots // 7 % 7 - 3
    dz = slots % 7 - 3
    parent = np.arange(8)
    px, py, pz = parent >> 2, parent >> 1 & 1, parent & 1
    wide = [d[:, None] + p[None, :] + 2 for d, p in ((dx, px), (dy, py), (dz, pz))]
    fine = np.ones((344, 8), bool)
    for d, p in ((dx, px), (dy, py), (dz, pz)):
        fine &= (d[:, None] >= -2 - p[None, :]) & (d[:, None] <= 3 - p[None, :])
    column = ((wide[0] // 2 * 3 + wide[2] // 2) * 3 + wide[1] // 2) * 8
    column = column + wide[0] % 2 * 4 + wide[1] % 2 * 2 + wide[2] % 2
    middle = np.where(fine, column, -1).reshape(-1)
    top = ((dx % 4) * 2 + dy % 2) * 4 + dz % 4
    hot = [
        (place[:, None] == np.arange(width)[None, :]).astype(np.float32).astype(jnp.bfloat16)
        for place, width in ((middle, 216), (top, 32))
    ]
    return jnp.asarray(hot[0]), jnp.asarray(hot[1])


def per_device(positions, charges, counts, moment_shift, far_operators, local_shift, lattice_operator):
    index = jnp.stack([lax.axis_index(axis) % 2 for axis in ("gx", "gy", "gz")]).astype(jnp.int32)
    pos = positions.reshape(3, 16, LANES)
    shift = moment_shift.transpose(1, 0, 2)
    local = local_shift.transpose(1, 0, 2)
    comb, low, high, middle, alone, live = make_moments()(
        pos, charges.reshape(16, LANES), counts.reshape(16, 4), shift
    )
    pick_middle, pick_top = selections()

    def exchange(axis, low, high):
        return shifted(high, axis, 1), shifted(low, axis, -1)

    def pack(block, *rest):
        return jnp.concatenate([block.reshape(-1, LANES), *rest], axis=0)

    left, right = exchange("gy", low, high)
    near_copy = jnp.concatenate([comb.reshape(LANES, LANES), middle, alone], axis=0)
    near_copy, alone = lax.optimization_barrier((near_copy, alone))
    wide_first = make_first()(far_operators, near_copy)
    above = shifted(alone, "gy", -2)
    blocks = near_copy[:128].reshape(2, 2, 2, 16, LANES)
    middle, alone = near_copy[128:136], near_copy[136:144]
    sides = [left[:64].reshape(2, 1, 2, 16, LANES), right[:64].reshape(2, 1, 2, 16, LANES)]
    blocks = jnp.concatenate([sides[0], blocks, sides[1]], axis=1)
    middle = jnp.concatenate([left[64:72], middle, right[64:72]], axis=0)
    line = jnp.concatenate(
        [left[72:73], alone[0:1], right[72:73], above[0:1], jnp.zeros((4, LANES), F32)], axis=0
    )

    sends = (pack(blocks[:, :, 0], middle, line), pack(blocks[:, :, 1], middle, line))
    sends, blocks, middle, line, wide_first = lax.optimization_barrier(
        (sends, blocks, middle, line, wide_first)
    )
    left, right = exchange("gz", *sends)
    wide_second, values, pick_upper, pick_child = make_second()(index, far_operators, pos, wide_first)
    sides = [left[:128].reshape(2, 4, 1, 16, LANES), right[:128].reshape(2, 4, 1, 16, LANES)]
    blocks = jnp.concatenate([sides[0], blocks, sides[1]], axis=2)
    middle = jnp.concatenate([left[128:152], middle, right[128:152]], axis=0)
    line = jnp.concatenate([left[152:160], line, right[152:160]], axis=0)

    sends = (pack(blocks[0], middle, line), pack(blocks[1], middle, line))
    sends, blocks, middle, line, wide_second = lax.optimization_barrier(
        (sends, blocks, middle, line, wide_second)
    )
    left, right = exchange("gx", *sends)
    mine, sums = make_inner()(blocks)

    sheet = jnp.concatenate([left[328:352], line, right[328:352]], axis=0)
    sheet, sums = lax.optimization_barrier((sheet, sums))
    sheet = jnp.concatenate([shifted(sheet, "gz", 3), sheet, shifted(sheet, "gz", -3)], axis=0)
    near = make_outer()(left, blocks, right, mine, sums)
    sheet, near = lax.optimization_barrier((sheet, near))
    upper_left = shifted(sheet, "gx", 3)
    upper_right = shifted(sheet, "gx", -3)

    wide_first, wide_second, middle_rows, leaf_rows = make_fetch()(
        wide_first, wide_second, pick_middle, left, blocks, right, middle, near
    )
    gradients = jnp.asarray(gradient_tables(), BF16)
    return make_far()(
        index,
        upper_left,
        sheet,
        upper_right,
        pick_top,
        shift,
        local,
        lattice_operator,
        gradients,
        near,
        wide_first,
        wide_second,
        values,
        pick_upper,
        pick_child,
        middle_rows,
        leaf_rows,
        live,
    )


def solution(mesh):
    placed = (
        P(None, "gx", "gy", "gz"),
        P("gx", "gy", "gz"),
        P("gx", "gy", "gz"),
        P(),
        P(),
        P(),
        P(),
    )
    return jax.shard_map(
        per_device,
        mesh=mesh,
        in_specs=placed,
        out_specs=(P("gx", "gy", "gz"), P(None, "gx", "gy", "gz")),
        check_vma=False,
    )
```

```python
import jax
import jax.numpy as jnp
import numpy as np
from jax import lax
from jax.experimental import pallas as pl
from jax.experimental.pallas import tpu as pltpu
from jax.sharding import PartitionSpec as P

ORDER = 8
TERMS = 81
SLOTS = 32
SOFTENING = 0.0625
LANES = 128
OFFSETS = 343
PLANE = 49 * LANES
F32 = jnp.float32
BF16 = jnp.bfloat16


def exponent_table():
    listed = []
    for accumulated in range(ORDER + 1):
        for height in (0, 1):
            for power_x in range(accumulated - height + 1):
                listed.append((power_x, accumulated - height - power_x, height))
    return listed


EXPONENTS = exponent_table()


def offset_rows():
    rows, count = [], 0
    for x in range(-3, 4):
        for y in range(-3, 4):
            for z in range(-3, 4):
                if max(abs(x), abs(y), abs(z)) >= 2:
                    rows.append(count)
                    count += 1
                else:
                    rows.append(-1)
    return rows


OFFSET_ROWS = offset_rows()


def gradient_tables():
    place = {e: k for k, e in enumerate(EXPONENTS)}
    tables = np.zeros((3, LANES, LANES), np.float32)
    for k, e in enumerate(EXPONENTS):
        for axis in range(3):
            if e[axis] > 0:
                lowered = list(e)
                lowered[axis] -= 1
                tables[axis, k, place[tuple(lowered)]] = e[axis]
    return tables


def full_spec(shape):
    return pl.BlockSpec(shape, lambda *_: (0,) * len(shape))


def nt_dot(left, right):
    return lax.dot_general(left, right, (((1,), (1,)), ((), ())), preferred_element_type=F32)


def split(value):
    upper = value.astype(BF16)
    lower = (value - upper.astype(F32)).astype(BF16)
    return upper, lower


def stack_split(value):
    upper = value.astype(BF16).astype(F32)
    return jnp.concatenate([upper, value - upper], axis=0).astype(BF16)


def apply_op(value, operator):
    both = nt_dot(stack_split(value)[:, :TERMS], operator)
    return both[:8] + both[8:]


def unpack_octants(source_ref, rows):
    rows[:, 0:TERMS] = source_ref[...].astype(F32).reshape(8 * TERMS, TERMS)


def octant_operator(rows, octant):
    return rows[pl.ds(octant, TERMS, stride=8), :][:, :TERMS].astype(BF16)


def iota(shape, axis):
    return lax.broadcasted_iota(jnp.int32, shape, axis)


def powers(value):
    listed = [None, value]
    for _ in range(2, ORDER + 1):
        listed.append(listed[-1] * value)
    return listed


def write_monomials(target, positions, factor):
    px = powers(positions[0] - 0.5)
    py = powers(positions[1] - 0.5)
    pz = positions[2] - 0.5
    for k, (a, b, c) in enumerate(EXPONENTS):
        value = factor
        if a:
            value = px[a] if value is None else value * px[a]
        if b:
            value = py[b] if value is None else value * py[b]
        if c:
            value = pz if value is None else value * pz
        if value is None:
            value = jnp.ones_like(pz)
        target[k * 16 : (k + 1) * 16, :] = value
    target[TERMS * 16 : LANES * 16, :] = jnp.zeros(((LANES - TERMS) * 16, LANES), F32)


def moments_kernel(
    pos_hbm,
    charge_hbm,
    count_hbm,
    shift_hbm,
    comb_ref,
    low_ref,
    high_ref,
    upper_ref,
    alone_ref,
    live_ref,
    pos_ref,
    charge_ref,
    count_ref,
    shift_ref,
    mono,
    leaf,
    rows,
    sems,
):
    loads = [
        pltpu.make_async_copy(a, b, sems.at[n])
        for n, (a, b) in enumerate(
            (
                (count_hbm, count_ref),
                (charge_hbm, charge_ref),
                (pos_hbm, pos_ref),
                (shift_hbm, shift_ref),
            )
        )
    ]
    for load in loads:
        load.start()
    for load in loads[:3]:
        load.wait()
    lane = iota((16, LANES), 1)
    count = jnp.zeros((16, LANES), jnp.int32)
    for z in range(4):
        count = jnp.where(lane // SLOTS == z, count_ref[:, z : z + 1], count)
    live = (lane % SLOTS < count).astype(F32)
    live_ref[...] = live
    weight = charge_ref[...] * live
    write_monomials(mono, (pos_ref[0], pos_ref[1], pos_ref[2]), weight)
    uppers, lowers = [], []
    for row in range(16):
        high, low = split(mono[pl.ds(row, LANES, stride=16), :])
        uppers.append(high)
        lowers.append(low)
    row = iota((64, 2048), 0)
    x = (row >> 5 & 1) * 2 + (row >> 2 & 1)
    y = (row >> 4 & 1) * 2 + (row >> 1 & 1)
    z = (row >> 3 & 1) * 2 + (row & 1)
    picker = (iota((64, 2048), 1) // SLOTS == (x * 4 + y) * 4 + z).astype(F32).astype(BF16)
    moments = nt_dot(picker, jnp.concatenate(uppers, axis=1)) + nt_dot(
        picker, jnp.concatenate(lowers, axis=1)
    )
    leaf[...] = moments
    comb_ref[:, 8:16, :] = moments.reshape(8, 8, LANES)
    lane8 = iota((8, LANES), 1)
    index = (iota((8, LANES), 0) % 4) * SLOTS + lane8 % SLOTS
    for xy in range(16):
        pieces = [pos_ref[c, xy : xy + 1, :] for c in range(3)] + [weight[xy : xy + 1, :]]
        merged = None
        for c, piece in enumerate(pieces):
            moved = jnp.take_along_axis(jnp.broadcast_to(piece, (8, LANES)), index, axis=1)
            merged = moved if merged is None else jnp.where(lane8 // SLOTS == c, moved, merged)
        cx, cy = xy // 4, xy % 4
        for half in range(2):
            parent = (cx // 2) * 4 + (cy // 2) * 2 + half
            inner = (cx % 2) * 4 + (cy % 2) * 2
            comb_ref[parent, inner : inner + 2, :] = merged[2 * half : 2 * half + 2, :]
    loads[3].wait()
    unpack_octants(shift_ref, rows)
    operators = [octant_operator(rows, octant) for octant in range(8)]
    upper_ref[...] = jnp.zeros((8, LANES), F32)
    middle = jnp.zeros((8, TERMS), F32)
    for octant in range(8):
        middle = middle + apply_op(leaf[pl.ds(octant, 8, stride=8), :], operators[octant])
    upper_ref[0:8, 0:TERMS] = middle
    wide = upper_ref[...]
    total = jnp.zeros((8, TERMS), F32)
    row8 = iota((8, TERMS), 0)
    for octant in range(8):
        total = total + jnp.where(row8 == octant, apply_op(wide, operators[octant]), 0.0)
    alone_ref[...] = jnp.zeros((8, LANES), F32)
    alone_ref[0:1, 0:TERMS] = jnp.sum(total, axis=0, keepdims=True)
    for half, target in enumerate((low_ref, high_ref)):
        for bx in range(2):
            for bz in range(2):
                at = 16 * (2 * bx + bz)
                target[at : at + 16, :] = comb_ref[4 * bx + 2 * half + bz]
        target[64:72, :] = upper_ref[...]
        target[72:80, :] = alone_ref[...]


def make_moments():
    return pl.pallas_call(
        moments_kernel,
        out_shape=(
            jax.ShapeDtypeStruct((8, 16, LANES), F32),
            jax.ShapeDtypeStruct((80, LANES), F32),
            jax.ShapeDtypeStruct((80, LANES), F32),
            jax.ShapeDtypeStruct((8, LANES), F32),
            jax.ShapeDtypeStruct((8, LANES), F32),
            jax.ShapeDtypeStruct((16, LANES), F32),
        ),
        in_specs=[pl.BlockSpec(memory_space=pl.ANY)] * 4,
        scratch_shapes=[
            pltpu.VMEM((3, 16, LANES), F32),
            pltpu.VMEM((16, LANES), F32),
            pltpu.VMEM((16, 4), jnp.int32),
            pltpu.VMEM((TERMS, 8, TERMS), BF16),
            pltpu.VMEM((LANES * 16, LANES), F32),
            pltpu.VMEM((64, LANES), F32),
            pltpu.VMEM((8 * TERMS, LANES), F32),
            pltpu.SemaphoreType.DMA((4,)),
        ],
        name="moments",
    )


UPPER_ROWS = 768
CUTS = [-(-row * TERMS // LANES) * LANES for row in (0, 49, 98, 138, 178, 218, 267)] + [25600]


def spot(relative_x, relative_z, relative_y):
    x = (relative_x + 3 & 7) + 1
    z = (relative_z + 3 & 7) + 1
    xb = x * 11 >> 5
    zb = z * 11 >> 5
    return xb * 216 + zb * 72 + (x - 3 * xb) * 24 + (z - 3 * zb) * 8 + (relative_y + 1 & 3)


def write_hot(target, column):
    rows = column.shape[0]
    lane = iota((rows, LANES), 1)
    for block in range(UPPER_ROWS // LANES):
        hot = (lane + block * LANES == column).astype(F32).astype(BF16)
        target[:, block * LANES : (block + 1) * LANES] = hot


def widen(far_hbm, wide_hbm, far_ref, wide_ref, sems, first, last):
    start = max(CUTS[first] - LANES, 0)
    edges = [start] + CUTS[first + 1 : last + 1]
    count = last - first
    loads = []
    for p in range(count):
        size = edges[p + 1] - edges[p]
        loads.append(
            pltpu.make_async_copy(
                far_hbm.at[:, pl.ds(edges[p], size)], far_ref.at[:, pl.ds(edges[p] - start, size)], sems.at[p]
            )
        )
    stores = []
    if wide_hbm is not None:
        stores = [
            pltpu.make_async_copy(wide_ref.at[p], wide_hbm.at[p], sems.at[count + p]) for p in range(count)
        ]
    for load in loads:
        load.start()

    def finish():
        lane = iota((TERMS, LANES), 1)
        for slot in range(49 * first, 49 * last):
            source = OFFSET_ROWS[slot]
            plane, inside = slot // 49 - first, slot % 49
            if inside == 0:
                loads[plane].wait()
            span = slice(inside * LANES, (inside + 1) * LANES)
            if source < 0:
                wide_ref[plane, :, span] = jnp.zeros((TERMS, LANES), BF16)
            else:
                base, shift = divmod(source * TERMS - start, LANES)
                merged = far_ref[:, base * LANES : (base + 1) * LANES]
                if shift + TERMS > LANES:
                    following = far_ref[:, (base + 1) * LANES : (base + 2) * LANES]
                    merged = jnp.where(lane >= shift, merged.astype(F32), following.astype(F32))
                    merged = merged.astype(BF16)
                if shift:
                    merged = pltpu.roll(merged, LANES - shift, 1)
                wide_ref[plane, :, span] = merged
            if inside == 48 and stores:
                stores[plane].start()
        for store in stores:
            store.wait()

    return finish


SPLITS = (0, 3, 6, 7)


def width_of(part):
    return CUTS[SPLITS[part + 1]] - max(CUTS[SPLITS[part]] - LANES, 0)


def first_kernel(far_hbm, after_ref, wide_hbm, far_ref, wide_ref, sems):
    widen(far_hbm, wide_hbm, far_ref, wide_ref, sems, SPLITS[0], SPLITS[1])()


def second_kernel(far_hbm, after_ref, wide_hbm, far_ref, wide_ref, sems):
    widen(far_hbm, wide_hbm, far_ref, wide_ref, sems, SPLITS[1], SPLITS[2])()


def write_picks(index_ref, upper_ref, child_ref):
    parity_x, parity_y, parity_z = index_ref[0], index_ref[1], index_ref[2]
    row = iota((256, LANES), 0)
    octant, box = row >> 5, row & 31
    vx = 2 * (box >> 3) + (octant >> 2) - parity_x
    vy = 2 * (box >> 2 & 1) + (octant >> 1 & 1) - parity_y
    vz = 2 * (box & 3) + (octant & 1) - parity_z
    write_hot(child_ref, spot(vx, vz, vy))
    row = iota((344, LANES), 0)
    plane = row * 1338 >> 16
    inside = row - plane * 49
    line = inside * 37 >> 8
    dx, dy, dz = plane - 3, line - 3, inside - line * 7 - 3
    fine = (dx >= -2 - parity_x) & (dx <= 3 - parity_x)
    fine = fine & (dy >= -2 - parity_y) & (dy <= 3 - parity_y)
    fine = fine & (dz >= -2 - parity_z) & (dz <= 3 - parity_z)
    write_hot(upper_ref, jnp.where(fine, spot(dx, dz, dy), -1))


def write_values(pos_ref, value_ref, mono):
    write_monomials(mono, (pos_ref[0], pos_ref[1], pos_ref[2]), None)
    for row in range(16):
        high, low = split(mono[pl.ds(row, LANES, stride=16), :])
        value_ref[0, :, row * LANES : (row + 1) * LANES] = high
        value_ref[1, :, row * LANES : (row + 1) * LANES] = low


VMEM_SPEC = pl.BlockSpec(memory_space=pltpu.VMEM)
HBM_SPEC = pl.BlockSpec(memory_space=pl.ANY)
SMEM_SPEC = pl.BlockSpec(memory_space=pltpu.SMEM)
WIDE = [jax.ShapeDtypeStruct((SPLITS[p + 1] - SPLITS[p], TERMS, PLANE), BF16) for p in range(3)]


def make_first():
    return pl.pallas_call(
        first_kernel,
        out_shape=WIDE[0],
        in_specs=[HBM_SPEC] * 2,
        out_specs=HBM_SPEC,
        scratch_shapes=[
            pltpu.VMEM((TERMS, width_of(0)), BF16),
            pltpu.VMEM(WIDE[0].shape, BF16),
            pltpu.SemaphoreType.DMA((6,)),
        ],
        name="first",
    )


def make_second():
    return pl.pallas_call(
        second_kernel,
        out_shape=WIDE[1],
        in_specs=[HBM_SPEC] * 2,
        out_specs=HBM_SPEC,
        scratch_shapes=[
            pltpu.VMEM((TERMS, width_of(1)), BF16),
            pltpu.VMEM(WIDE[1].shape, BF16),
            pltpu.SemaphoreType.DMA((6,)),
        ],
        name="second",
    )


def fill_window(window, left_ref, own_ref, right_ref, first_row):
    for bx in range(4):
        for by in range(4):
            for bz in range(4):
                if bx in (1, 2):
                    tile = own_ref[bx - 1, by, bz, first_row : first_row + 8, :]
                else:
                    at = 16 * (4 * by + bz) + first_row
                    tile = (left_ref if bx == 0 else right_ref)[at : at + 8, :]
                for i in range(2):
                    for j in range(2):
                        inner = i * 4 + j * 2
                        window[2 * bx + i, 2 * by + j, 2 * bz : 2 * bz + 2, :] = tile[inner : inner + 2, :]


def fill_slab(window, slab, tile, inner):
    for by in range(4):
        for bz in range(4):
            rows = tile(by, bz)
            for j in range(2):
                at = inner * 4 + j * 2
                window[slab, 2 * by + j, 2 * bz : 2 * bz + 2, :] = rows[at : at + 2, :]


def spread_slabs(window, rolled, spread, slabs, used):
    row8 = iota((8, LANES), 0)
    for x in range(slabs):
        for dz in range(3):
            for pair in range(3):
                first = pltpu.roll(window[x, 2 * pair + 1], 7 - dz, 0)
                second = pltpu.roll(window[x, 2 * pair + 2], (7 - dz + 4) % 8, 0)
                at = (x * 3 + dz) * 24 + 8 * pair
                rolled[at : at + 8, :] = jnp.where(row8 < 4, first, second)
    value = rolled[0 : used * 72, :]
    high = value.astype(BF16)
    rest = value - high.astype(F32)
    middle = rest.astype(BF16)
    low = (rest - middle.astype(F32)).astype(BF16)
    pieces = jnp.concatenate([high, middle, low], axis=1)
    column = iota((LANES, 2 * LANES), 1)
    row = iota((LANES, 2 * LANES), 0)
    for block in range(16):
        group, half = block // 2, block % 2
        wanted = (column // LANES + 2 * half) * SLOTS + 4 * group + column % LANES // SLOTS
        hot = (row == wanted).astype(F32).astype(BF16)
        found = jnp.dot(pieces, jnp.concatenate([hot, hot, hot], axis=0), preferred_element_type=F32)
        spread[2 * block] = found[:, 0:LANES]
        spread[2 * block + 1] = found[:, LANES : 2 * LANES]


def add_slab(mine, shift, spread, base, sums):
    tx = mine[0] - shift
    pot, fx, fy, fz = sums
    for ey in range(3):
        ty = mine[1] - float(ey - 1)
        for ez in range(3):
            tz = mine[2] - float(ez - 1)
            at = base + (ez * 24 + 4 * ey)
            for group in range(8):
                dx = tx - spread[4 * group, pl.ds(at, 16), :]
                dy = ty - spread[4 * group + 1, pl.ds(at, 16), :]
                dz = tz - spread[4 * group + 2, pl.ds(at, 16), :]
                inverse = lax.rsqrt(dx * dx + dy * dy + dz * dz + SOFTENING)
                weight = spread[4 * group + 3, pl.ds(at, 16), :] * inverse
                cubic = weight * (inverse * inverse)
                pot = pot + weight
                fx = fx + cubic * dx
                fy = fy + cubic * dy
                fz = fz + cubic * dz
    return pot, fx, fy, fz


def inner_kernel(own_ref, mine_ref, sum_ref, window, rolled, spread):
    for x in range(4):
        fill_slab(window, x, lambda by, bz: own_ref[x // 2, by, bz, 0:8, :], x % 2)
    spread_slabs(window, rolled, spread, 4, 3)
    slot = iota((16, LANES), 1) % SLOTS
    for x in range(4):
        own = rolled[(x * 3 + 1) * 24 + 4 : (x * 3 + 1) * 24 + 20, :]
        for c in range(4):
            mine_ref[x, c] = jnp.take_along_axis(own, c * SLOTS + slot, axis=1)
    sum_ref[...] = jnp.zeros((4, 4, 16, LANES), F32)

    def one_pair(step, carry):
        source = (step + 1) // 3
        shift = 1 - ((step + 1) - 3 * source)
        target = source - shift
        mine = [mine_ref[target, c] for c in range(3)]
        base = source * 72
        sums = tuple(sum_ref[target, c] for c in range(4))
        sums = add_slab(mine, shift.astype(F32), spread, base, sums)
        for c in range(4):
            sum_ref[target, c] = sums[c]
        return carry

    lax.fori_loop(0, 8, one_pair, 0)


def make_inner():
    return pl.pallas_call(
        inner_kernel,
        out_shape=(
            jax.ShapeDtypeStruct((4, 4, 16, LANES), F32),
            jax.ShapeDtypeStruct((4, 4, 16, LANES), F32),
        ),
        scratch_shapes=[
            pltpu.VMEM((4, 8, 8, LANES), F32),
            pltpu.VMEM((288, LANES), F32),
            pltpu.VMEM((32, 216, LANES), F32),
        ],
        compiler_params=pltpu.CompilerParams(vmem_limit_bytes=40 << 20),
        name="inner",
    )


def outer_kernel(left_ref, own_ref, right_ref, mine_ref, sum_ref, near_ref, sums_ref, window, rolled, spread):
    fill_slab(window, 0, lambda by, bz: left_ref[16 * (4 * by + bz) : 16 * (4 * by + bz) + 8, :], 1)
    fill_slab(window, 1, lambda by, bz: right_ref[16 * (4 * by + bz) : 16 * (4 * by + bz) + 8, :], 0)
    fill_slab(window, 2, lambda by, bz: own_ref[1, by, bz, 0:8, :], 1)
    spread_slabs(window, rolled, spread, 3, 3)
    sums_ref[...] = sum_ref[...]

    def one_pair(step, carry):
        target = jnp.where(step == 0, 0, jnp.where(step == 1, 2, 3))
        slab = jnp.where(step == 0, 0, jnp.where(step == 3, 1, 2))
        shift = jnp.where(step == 0, -1, jnp.where(step == 2, 0, 1))
        mine = [mine_ref[target, c] for c in range(3)]
        sums = tuple(sums_ref[target, c] for c in range(4))
        sums = add_slab(mine, shift.astype(F32), spread, slab * 72, sums)
        for c in range(4):
            sums_ref[target, c] = sums[c]
        return carry

    lax.fori_loop(0, 4, one_pair, 0)
    part = iota((16, LANES), 1) // SLOTS
    keep = part == iota((16, LANES), 0) % 4
    itself = lax.rsqrt(jnp.full((16, LANES), SOFTENING, F32))

    for x in range(4):
        totals = []
        for c in range(4):
            value = sums_ref[x, c]
            value = value + pltpu.roll(value, 64, 1)
            value = value + pltpu.roll(value, 32, 1)
            totals.append(value)
        totals[0] = totals[0] - mine_ref[x, 3] * itself
        for c in range(4):
            chosen = jnp.where(keep, totals[c], 0.0)
            rows = [jnp.sum(chosen[4 * y : 4 * y + 4], axis=0, keepdims=True) for y in range(4)]
            near_ref[c, x] = jnp.concatenate(rows, axis=0)


def make_outer():
    return pl.pallas_call(
        outer_kernel,
        out_shape=jax.ShapeDtypeStruct((4, 4, 4, LANES), F32),
        scratch_shapes=[
            pltpu.VMEM((4, 4, 16, LANES), F32),
            pltpu.VMEM((3, 8, 8, LANES), F32),
            pltpu.VMEM((216, LANES), F32),
            pltpu.VMEM((32, 216, LANES), F32),
        ],
        compiler_params=pltpu.CompilerParams(vmem_limit_bytes=40 << 20),
        name="outer",
    )


def two(value):
    return jnp.concatenate(split(value), axis=1)


def fetch_kernel(
    index_ref,
    far_hbm,
    first_hbm,
    second_hbm,
    pos_ref,
    pick_middle_ref,
    left_ref,
    own_ref,
    right_ref,
    middle_ref,
    after_ref,
    wide_first_ref,
    wide_second_ref,
    wide_third_ref,
    middle_rows,
    leaf_rows,
    value_ref,
    pick_upper_ref,
    pick_child_ref,
    window,
    rolled,
    mono,
    far_ref,
    sems,
):
    finish = widen(far_hbm, None, far_ref, wide_third_ref, sems, SPLITS[2], SPLITS[3])
    copies = [
        pltpu.make_async_copy(first_hbm, wide_first_ref, sems.at[1]),
        pltpu.make_async_copy(second_hbm, wide_second_ref, sems.at[2]),
    ]
    for copy in copies:
        copy.start()
    fill_window(window, left_ref, own_ref, right_ref, 8)
    row8 = iota((8, LANES), 0)
    row16 = iota((16, LANES), 0)
    rolled[:, 0:8, :] = jnp.zeros((7, 8, LANES), F32)
    rolled[:, 40:48, :] = jnp.zeros((7, 8, LANES), F32)

    def gather_plane(x, carry):
        for dz in range(-3, 4):
            for pair in range(4):
                even = pltpu.roll(window[x, 2 * pair], (16 - (dz + 2)) % 8, 0)
                odd = pltpu.roll(window[x, 2 * pair + 1], (16 - (dz + 2) + 4) % 8, 0)
                value = jnp.where(row8 < 4, even, odd)
                if dz == -3:
                    value = jnp.where(row8 % 2 == 1, value, 0.0)
                if dz == 3:
                    value = jnp.where(row8 % 2 == 0, value, 0.0)
                rolled[dz + 3, 8 + 8 * pair : 16 + 8 * pair, :] = value
        for dy in range(-3, 4):
            for dz in range(-3, 4):
                start = 8 + 4 * (dy + 2)
                value = rolled[dz + 3, start : start + 16, :]
                if dy == -3:
                    value = jnp.where(row16 // 4 % 2 == 1, value, 0.0)
                if dy == 3:
                    value = jnp.where(row16 // 4 % 2 == 0, value, 0.0)
                high, low = split(value)
                at = ((dy + 3) * 7 + dz + 3) * LANES
                leaf_rows[x, 0:16, at : at + LANES] = high
                leaf_rows[x, 16:32, at : at + LANES] = low
        return carry

    lax.fori_loop(0, 8, gather_plane, 0)
    middles = two(
        jnp.concatenate([left_ref[256:328, :], middle_ref[...], right_ref[256:328, :]], axis=0)
    )

    def middle_plane(p, carry):
        rows = pick_middle_ref[pl.ds(pl.multiple_of(p * 392, 8), 392), :]
        found = jnp.dot(rows, middles, preferred_element_type=F32)
        for inside in range(49):
            piece = found[8 * inside : 8 * inside + 8]
            middle_rows[p, :, inside * LANES : (inside + 1) * LANES] = jnp.concatenate(
                [piece[:, 0:LANES], piece[:, LANES : 2 * LANES]], axis=0
            ).astype(BF16)
        return carry

    lax.fori_loop(0, 7, middle_plane, 0)
    write_picks(index_ref, pick_upper_ref, pick_child_ref)
    write_values(pos_ref, value_ref, mono)
    finish()
    for copy in copies:
        copy.wait()


FETCHED = (
    *WIDE,
    jax.ShapeDtypeStruct((7, 16, PLANE), BF16),
    jax.ShapeDtypeStruct((8, 32, PLANE), BF16),
    jax.ShapeDtypeStruct((2, LANES, 2048), BF16),
    jax.ShapeDtypeStruct((344, UPPER_ROWS), BF16),
    jax.ShapeDtypeStruct((256, UPPER_ROWS), BF16),
)


def make_fetch():
    return pl.pallas_call(
        fetch_kernel,
        out_shape=FETCHED,
        in_specs=[SMEM_SPEC] + [HBM_SPEC] * 3 + [VMEM_SPEC] * 6 + [HBM_SPEC],
        out_specs=(VMEM_SPEC,) * len(FETCHED),
        scratch_shapes=[
            pltpu.VMEM((8, 8, 8, LANES), F32),
            pltpu.VMEM((7, 48, LANES), F32),
            pltpu.VMEM((LANES * 16, LANES), F32),
            pltpu.VMEM((TERMS, width_of(2)), BF16),
            pltpu.SemaphoreType.DMA((3,)),
        ],
        compiler_params=pltpu.CompilerParams(vmem_limit_bytes=FETCH_LIMIT << 20),
        name="fetch",
    )


FETCH_LIMIT = 36


def far_kernel(
    index_ref,
    upper_left_ref,
    upper_own_ref,
    upper_right_ref,
    pick_top_ref,
    shift_ref,
    local_ref,
    lattice_ref,
    gradient_ref,
    near_ref,
    wide_first_ref,
    wide_second_ref,
    wide_third_ref,
    middle_rows,
    leaf_rows,
    value_ref,
    pick_upper_ref,
    pick_child_ref,
    live_ref,
    potential_ref,
    field_ref,
    few_rows,
    few,
    top,
    acc,
    local,
    shift_rows,
    local_rows,
):
    unpack_octants(shift_ref, shift_rows)
    unpack_octants(local_ref, local_rows)
    uppers = two(
        jnp.concatenate(
            [
                upper_left_ref[...],
                upper_own_ref[...],
                upper_right_ref[...],
                jnp.zeros((UPPER_ROWS - 648, LANES), F32),
            ],
            axis=0,
        )
    )
    children = jnp.dot(pick_child_ref[...], uppers, preferred_element_type=F32)
    total = jnp.zeros((32, TERMS), F32)
    for octant in range(8):
        rows = children[32 * octant : 32 * octant + 32]
        both = jnp.concatenate([rows[:, :TERMS], rows[:, LANES : LANES + TERMS]], axis=0).astype(BF16)
        made = nt_dot(both, octant_operator(shift_rows, octant))
        total = total + made[:32] + made[32:]
    top[...] = jnp.zeros((32, LANES), F32)
    top[:, 0:TERMS] = total
    few[...] = jnp.zeros((OFFSETS * 8 + 8, LANES), F32)
    from_upper = jnp.dot(pick_upper_ref[...], uppers, preferred_element_type=F32)
    from_top = jnp.dot(pick_top_ref[...], two(top[...]), preferred_element_type=F32)
    for side in range(2):
        span = slice(side * LANES, (side + 1) * LANES)
        few[pl.ds(2 * side, 344, stride=8), :] = from_upper[:, span]
        few[pl.ds(2 * side + 1, 344, stride=8), :] = from_top[:, span]
    none = jnp.zeros((8, LANES), F32)

    def few_plane(p, carry):
        for inside in range(49):
            rows = few[pl.ds(pl.multiple_of(p * 392 + inside * 8, 8), 8), :]
            few_rows[p, :, inside * LANES : (inside + 1) * LANES] = jnp.concatenate(
                [rows, none], axis=0
            ).astype(BF16)
        return carry

    lax.fori_loop(0, 7, few_plane, 0)

    acc[...] = jnp.zeros((160, LANES), F32)
    for p in range(7):
        if p == 0:
            parts, places = [0, 2], [1, 3]
        elif p == 6:
            parts, places = [5, 7], [0, 2]
        else:
            parts, places = None, None
        if parts is None:
            left = leaf_rows[p - 1 : p + 3].reshape(128, PLANE)
        else:
            left = jnp.concatenate([leaf_rows[q] for q in parts], axis=0)
        left = jnp.concatenate([left, middle_rows[p], few_rows[p]], axis=0)
        part = p // 3
        right = (wide_first_ref, wide_second_ref, wide_third_ref)[part][p - SPLITS[part]]
        found = nt_dot(left, right)
        if parts is None:
            acc[:, 0:TERMS] += found
        else:
            for n, place in enumerate(places):
                acc[32 * place : 32 * place + 32, 0:TERMS] += found[32 * n : 32 * n + 32]
            acc[128:160, 0:TERMS] += found[64:96]

    far_middle = acc[128:136, :] + acc[136:144, :]
    far_rest = acc[144:146, :] + acc[146:148, :]
    root = jnp.sum(top[...], axis=0, keepdims=True)
    local[...] = jnp.zeros((8, LANES), F32)
    lattice = apply_op(jnp.broadcast_to(root, (8, LANES)), lattice_ref[...])
    local[:, 0:TERMS] = 0.125 * (far_rest[1:2, 0:TERMS] + lattice)
    own = index_ref[0] * 4 + index_ref[1] * 2 + index_ref[2]
    lowered = apply_op(local[...], octant_operator(local_rows, own))
    local[:, 0:TERMS] = 0.25 * far_rest[0:1, 0:TERMS] + lowered
    row_terms = iota((8, TERMS), 0)
    upper_local = local[...]
    spread = jnp.zeros((8, TERMS), F32)
    for octant in range(8):
        spread = spread + jnp.where(row_terms == octant, apply_op(upper_local, octant_operator(local_rows, octant)), 0.0)
    local[:, 0:TERMS] = 0.5 * far_middle[:, 0:TERMS] + spread
    middle_local = local[...]
    for x in range(4):
        base = 32 * x
        acc[base : base + 16, :] = acc[base : base + 16, :] + acc[base + 16 : base + 32, :]
    for octant in range(8):
        i, j, l = octant >> 2, octant >> 1 & 1, octant & 1
        made = apply_op(middle_local, octant_operator(local_rows, octant))
        for parent in range(8):
            bx, by, bz = parent >> 2, parent >> 1 & 1, parent & 1
            at = 32 * (2 * bx + i) + 4 * (2 * by + j) + 2 * bz + l
            acc[at : at + 1, 0:TERMS] += made[parent : parent + 1]
    for x in range(4):
        base = acc[32 * x : 32 * x + 16, :]
        high, low = split(base)
        both = jnp.concatenate([high, low], axis=0)
        listed = [base]
        for axis in range(3):
            made = jnp.dot(both, gradient_ref[axis], preferred_element_type=F32)
            listed.append(-(made[:16] + made[16:]))
        high, low = split(jnp.concatenate(listed, axis=0))
        first = value_ref[0, :, 512 * x : 512 * x + 512]
        second = value_ref[1, :, 512 * x : 512 * x + 512]
        found = jnp.dot(jnp.concatenate([high, low], axis=0), first, preferred_element_type=F32)
        found = found[:64] + found[64:] + jnp.dot(high, second, preferred_element_type=F32)
        keep = iota((4, LANES), 1) // SLOTS == iota((4, LANES), 0)
        for c in range(4):
            rows = []
            for y in range(4):
                piece = found[16 * c + 4 * y : 16 * c + 4 * y + 4, LANES * y : LANES * y + LANES]
                rows.append(jnp.sum(jnp.where(keep, piece, 0.0), axis=0, keepdims=True))
            value = (near_ref[c, x] + jnp.concatenate(rows, axis=0)) * live_ref[4 * x : 4 * x + 4, :]
            if c == 0:
                potential_ref[x] = value
            else:
                field_ref[c - 1, x] = value


def make_far():
    return pl.pallas_call(
        far_kernel,
        out_shape=(
            jax.ShapeDtypeStruct((4, 4, LANES), F32),
            jax.ShapeDtypeStruct((3, 4, 4, LANES), F32),
        ),
        in_specs=[SMEM_SPEC] + [VMEM_SPEC] * 18,
        scratch_shapes=[
            pltpu.VMEM((7, 16, PLANE), BF16),
            pltpu.VMEM((OFFSETS * 8 + 8, LANES), F32),
            pltpu.VMEM((32, LANES), F32),
            pltpu.VMEM((160, LANES), F32),
            pltpu.VMEM((8, LANES), F32),
            pltpu.VMEM((8 * TERMS, LANES), F32),
            pltpu.VMEM((8 * TERMS, LANES), F32),
        ],
        compiler_params=pltpu.CompilerParams(vmem_limit_bytes=24 << 20),
        name="far",
    )


def shifted(value, axis, shift):
    count = lax.axis_size(axis)
    return lax.ppermute(value, axis, [(i, (i + shift) % count) for i in range(count)])


def selections():
    slots = np.arange(344)
    dx = np.minimum(slots // 49, 6) - 3
    dy = slots // 7 % 7 - 3
    dz = slots % 7 - 3
    parent = np.arange(8)
    px, py, pz = parent >> 2, parent >> 1 & 1, parent & 1
    wide = [d[:, None] + p[None, :] + 2 for d, p in ((dx, px), (dy, py), (dz, pz))]
    fine = np.ones((344, 8), bool)
    for d, p in ((dx, px), (dy, py), (dz, pz)):
        fine &= (d[:, None] >= -2 - p[None, :]) & (d[:, None] <= 3 - p[None, :])
    column = ((wide[0] // 2 * 3 + wide[2] // 2) * 3 + wide[1] // 2) * 8
    column = column + wide[0] % 2 * 4 + wide[1] % 2 * 2 + wide[2] % 2
    middle = np.where(fine, column, -1).reshape(-1)
    top = ((dx % 4) * 2 + dy % 2) * 4 + dz % 4
    hot = [
        (place[:, None] == np.arange(width)[None, :]).astype(np.float32).astype(jnp.bfloat16)
        for place, width in ((middle, 216), (top, 32))
    ]
    return jnp.asarray(hot[0]), jnp.asarray(hot[1])


def per_device(positions, charges, counts, moment_shift, far_operators, local_shift, lattice_operator):
    index = jnp.stack([lax.axis_index(axis) % 2 for axis in ("gx", "gy", "gz")]).astype(jnp.int32)
    pos = positions.reshape(3, 16, LANES)
    shift = moment_shift.transpose(1, 0, 2)
    local = local_shift.transpose(1, 0, 2)
    comb, low, high, middle, alone, live = make_moments()(
        pos, charges.reshape(16, LANES), counts.reshape(16, 4), shift
    )
    pick_middle, pick_top = selections()

    def exchange(axis, low, high):
        return shifted(high, axis, 1), shifted(low, axis, -1)

    def pack(block, *rest):
        return jnp.concatenate([block.reshape(-1, LANES), *rest], axis=0)

    left, right = exchange("gy", low, high)
    above = shifted(alone, "gy", -2)
    near_copy = jnp.concatenate([comb.reshape(LANES, LANES), middle, alone], axis=0)
    near_copy = lax.optimization_barrier(near_copy)
    wide_first = make_first()(far_operators, alone)
    blocks = near_copy[:128].reshape(2, 2, 2, 16, LANES)
    middle, alone = near_copy[128:136], near_copy[136:144]
    sides = [left[:64].reshape(2, 1, 2, 16, LANES), right[:64].reshape(2, 1, 2, 16, LANES)]
    blocks = jnp.concatenate([sides[0], blocks, sides[1]], axis=1)
    middle = jnp.concatenate([left[64:72], middle, right[64:72]], axis=0)
    line = jnp.concatenate(
        [left[72:73], alone[0:1], right[72:73], above[0:1], jnp.zeros((4, LANES), F32)], axis=0
    )

    sends = (pack(blocks[:, :, 0], middle, line), pack(blocks[:, :, 1], middle, line))
    sends, blocks, middle, line, wide_first = lax.optimization_barrier(
        (sends, blocks, middle, line, wide_first)
    )
    left, right = exchange("gz", *sends)
    wide_second = make_second()(far_operators, wide_first)
    sides = [left[:128].reshape(2, 4, 1, 16, LANES), right[:128].reshape(2, 4, 1, 16, LANES)]
    blocks = jnp.concatenate([sides[0], blocks, sides[1]], axis=2)
    middle = jnp.concatenate([left[128:152], middle, right[128:152]], axis=0)
    line = jnp.concatenate([left[152:160], line, right[152:160]], axis=0)

    sends = (pack(blocks[0], middle, line), pack(blocks[1], middle, line))
    sends, blocks, middle, line, wide_second = lax.optimization_barrier(
        (sends, blocks, middle, line, wide_second)
    )
    left, right = exchange("gx", *sends)
    mine, sums = make_inner()(blocks)

    sheet = jnp.concatenate([left[328:352], line, right[328:352]], axis=0)
    sheet, sums = lax.optimization_barrier((sheet, sums))
    sheet = jnp.concatenate([shifted(sheet, "gz", 3), sheet, shifted(sheet, "gz", -3)], axis=0)
    near = make_outer()(left, blocks, right, mine, sums)
    sheet, near = lax.optimization_barrier((sheet, near))
    upper_left = shifted(sheet, "gx", 3)
    upper_right = shifted(sheet, "gx", -3)

    prepared = make_fetch()(
        index, far_operators, wide_first, wide_second, pos, pick_middle, left, blocks, right, middle, near
    )
    gradients = jnp.asarray(gradient_tables(), BF16)
    return make_far()(
        index,
        upper_left,
        sheet,
        upper_right,
        pick_top,
        shift,
        local,
        lattice_operator,
        gradients,
        near,
        *prepared,
        live,
    )


def solution(mesh):
    placed = (
        P(None, "gx", "gy", "gz"),
        P("gx", "gy", "gz"),
        P("gx", "gy", "gz"),
        P(),
        P(),
        P(),
        P(),
    )
    return jax.shard_map(
        per_device,
        mesh=mesh,
        in_specs=placed,
        out_specs=(P("gx", "gy", "gz"), P(None, "gx", "gy", "gz")),
        check_vma=False,
    )
```

```python
import jax
import jax.numpy as jnp
import numpy as np
from jax import lax
from jax.experimental import pallas as pl
from jax.experimental.pallas import tpu as pltpu
from jax.sharding import PartitionSpec as P

ORDER = 8
TERMS = 81
SLOTS = 32
SOFTENING = 0.0625
LANES = 128
OFFSETS = 343
PLANE = 49 * LANES
F32 = jnp.float32
BF16 = jnp.bfloat16


def exponent_table():
    listed = []
    for accumulated in range(ORDER + 1):
        for height in (0, 1):
            for power_x in range(accumulated - height + 1):
                listed.append((power_x, accumulated - height - power_x, height))
    return listed


EXPONENTS = exponent_table()


def offset_rows():
    rows, count = [], 0
    for x in range(-3, 4):
        for y in range(-3, 4):
            for z in range(-3, 4):
                if max(abs(x), abs(y), abs(z)) >= 2:
                    rows.append(count)
                    count += 1
                else:
                    rows.append(-1)
    return rows


OFFSET_ROWS = offset_rows()


def gradient_tables():
    place = {e: k for k, e in enumerate(EXPONENTS)}
    tables = np.zeros((3, LANES, LANES), np.float32)
    for k, e in enumerate(EXPONENTS):
        for axis in range(3):
            if e[axis] > 0:
                lowered = list(e)
                lowered[axis] -= 1
                tables[axis, k, place[tuple(lowered)]] = e[axis]
    return tables


def full_spec(shape):
    return pl.BlockSpec(shape, lambda *_: (0,) * len(shape))


def nt_dot(left, right):
    return lax.dot_general(left, right, (((1,), (1,)), ((), ())), preferred_element_type=F32)


def split(value):
    upper = value.astype(BF16)
    lower = (value - upper.astype(F32)).astype(BF16)
    return upper, lower


def stack_split(value):
    upper = value.astype(BF16).astype(F32)
    return jnp.concatenate([upper, value - upper], axis=0).astype(BF16)


def apply_op(value, operator):
    both = nt_dot(stack_split(value)[:, :TERMS], operator)
    return both[:8] + both[8:]


def unpack_octants(source_ref, rows):
    rows[:, 0:TERMS] = source_ref[...].astype(F32).reshape(8 * TERMS, TERMS)


def octant_operator(rows, octant):
    return rows[pl.ds(octant, TERMS, stride=8), :][:, :TERMS].astype(BF16)


def iota(shape, axis):
    return lax.broadcasted_iota(jnp.int32, shape, axis)


def powers(value):
    listed = [None, value]
    for _ in range(2, ORDER + 1):
        listed.append(listed[-1] * value)
    return listed


def write_monomials(target, positions, factor):
    px = powers(positions[0] - 0.5)
    py = powers(positions[1] - 0.5)
    pz = positions[2] - 0.5
    for k, (a, b, c) in enumerate(EXPONENTS):
        value = factor
        if a:
            value = px[a] if value is None else value * px[a]
        if b:
            value = py[b] if value is None else value * py[b]
        if c:
            value = pz if value is None else value * pz
        if value is None:
            value = jnp.ones_like(pz)
        target[k * 16 : (k + 1) * 16, :] = value
    target[TERMS * 16 : LANES * 16, :] = jnp.zeros(((LANES - TERMS) * 16, LANES), F32)


def moments_kernel(
    pos_hbm,
    charge_hbm,
    count_hbm,
    shift_hbm,
    comb_ref,
    low_ref,
    high_ref,
    upper_ref,
    alone_ref,
    live_ref,
    pos_ref,
    charge_ref,
    count_ref,
    shift_ref,
    mono,
    leaf,
    rows,
    sems,
):
    loads = [
        pltpu.make_async_copy(a, b, sems.at[n])
        for n, (a, b) in enumerate(
            (
                (count_hbm, count_ref),
                (charge_hbm, charge_ref),
                (pos_hbm, pos_ref),
                (shift_hbm, shift_ref),
            )
        )
    ]
    for load in loads:
        load.start()
    for load in loads[:3]:
        load.wait()
    lane = iota((16, LANES), 1)
    count = jnp.zeros((16, LANES), jnp.int32)
    for z in range(4):
        count = jnp.where(lane // SLOTS == z, count_ref[:, z : z + 1], count)
    live = (lane % SLOTS < count).astype(F32)
    live_ref[...] = live
    weight = charge_ref[...] * live
    write_monomials(mono, (pos_ref[0], pos_ref[1], pos_ref[2]), weight)
    uppers, lowers = [], []
    for row in range(16):
        high, low = split(mono[pl.ds(row, LANES, stride=16), :])
        uppers.append(high)
        lowers.append(low)
    row = iota((64, 2048), 0)
    x = (row >> 5 & 1) * 2 + (row >> 2 & 1)
    y = (row >> 4 & 1) * 2 + (row >> 1 & 1)
    z = (row >> 3 & 1) * 2 + (row & 1)
    picker = (iota((64, 2048), 1) // SLOTS == (x * 4 + y) * 4 + z).astype(F32).astype(BF16)
    moments = nt_dot(picker, jnp.concatenate(uppers, axis=1)) + nt_dot(
        picker, jnp.concatenate(lowers, axis=1)
    )
    leaf[...] = moments
    comb_ref[:, 8:16, :] = moments.reshape(8, 8, LANES)
    lane8 = iota((8, LANES), 1)
    index = (iota((8, LANES), 0) % 4) * SLOTS + lane8 % SLOTS
    for xy in range(16):
        pieces = [pos_ref[c, xy : xy + 1, :] for c in range(3)] + [weight[xy : xy + 1, :]]
        merged = None
        for c, piece in enumerate(pieces):
            moved = jnp.take_along_axis(jnp.broadcast_to(piece, (8, LANES)), index, axis=1)
            merged = moved if merged is None else jnp.where(lane8 // SLOTS == c, moved, merged)
        cx, cy = xy // 4, xy % 4
        for half in range(2):
            parent = (cx // 2) * 4 + (cy // 2) * 2 + half
            inner = (cx % 2) * 4 + (cy % 2) * 2
            comb_ref[parent, inner : inner + 2, :] = merged[2 * half : 2 * half + 2, :]
    loads[3].wait()
    unpack_octants(shift_ref, rows)
    operators = [octant_operator(rows, octant) for octant in range(8)]
    upper_ref[...] = jnp.zeros((8, LANES), F32)
    middle = jnp.zeros((8, TERMS), F32)
    for octant in range(8):
        middle = middle + apply_op(leaf[pl.ds(octant, 8, stride=8), :], operators[octant])
    upper_ref[0:8, 0:TERMS] = middle
    wide = upper_ref[...]
    total = jnp.zeros((8, TERMS), F32)
    row8 = iota((8, TERMS), 0)
    for octant in range(8):
        total = total + jnp.where(row8 == octant, apply_op(wide, operators[octant]), 0.0)
    alone_ref[...] = jnp.zeros((8, LANES), F32)
    alone_ref[0:1, 0:TERMS] = jnp.sum(total, axis=0, keepdims=True)
    for half, target in enumerate((low_ref, high_ref)):
        for bx in range(2):
            for bz in range(2):
                at = 16 * (2 * bx + bz)
                target[at : at + 16, :] = comb_ref[4 * bx + 2 * half + bz]
        target[64:72, :] = upper_ref[...]
        target[72:80, :] = alone_ref[...]


def make_moments():
    return pl.pallas_call(
        moments_kernel,
        out_shape=(
            jax.ShapeDtypeStruct((8, 16, LANES), F32),
            jax.ShapeDtypeStruct((80, LANES), F32),
            jax.ShapeDtypeStruct((80, LANES), F32),
            jax.ShapeDtypeStruct((8, LANES), F32),
            jax.ShapeDtypeStruct((8, LANES), F32),
            jax.ShapeDtypeStruct((16, LANES), F32),
        ),
        in_specs=[pl.BlockSpec(memory_space=pl.ANY)] * 4,
        scratch_shapes=[
            pltpu.VMEM((3, 16, LANES), F32),
            pltpu.VMEM((16, LANES), F32),
            pltpu.VMEM((16, 4), jnp.int32),
            pltpu.VMEM((TERMS, 8, TERMS), BF16),
            pltpu.VMEM((LANES * 16, LANES), F32),
            pltpu.VMEM((64, LANES), F32),
            pltpu.VMEM((8 * TERMS, LANES), F32),
            pltpu.SemaphoreType.DMA((4,)),
        ],
        name="moments",
    )


UPPER_ROWS = 768
CUTS = [-(-row * TERMS // LANES) * LANES for row in (0, 49, 98, 138, 178, 218, 267)] + [25600]


def spot(relative_x, relative_z, relative_y):
    x = (relative_x + 3 & 7) + 1
    z = (relative_z + 3 & 7) + 1
    xb = x * 11 >> 5
    zb = z * 11 >> 5
    return xb * 216 + zb * 72 + (x - 3 * xb) * 24 + (z - 3 * zb) * 8 + (relative_y + 1 & 3)


def write_hot(target, column):
    rows = column.shape[0]
    lane = iota((rows, LANES), 1)
    for block in range(UPPER_ROWS // LANES):
        hot = (lane + block * LANES == column).astype(F32).astype(BF16)
        target[:, block * LANES : (block + 1) * LANES] = hot


def widen(far_hbm, wide_hbm, far_ref, wide_ref, sems, first, last):
    start = max(CUTS[first] - LANES, 0)
    edges = [start] + CUTS[first + 1 : last + 1]
    count = last - first
    loads = []
    for p in range(count):
        size = edges[p + 1] - edges[p]
        loads.append(
            pltpu.make_async_copy(
                far_hbm.at[:, pl.ds(edges[p], size)], far_ref.at[:, pl.ds(edges[p] - start, size)], sems.at[p]
            )
        )
    stores = []
    if wide_hbm is not None:
        stores = [
            pltpu.make_async_copy(wide_ref.at[p], wide_hbm.at[p], sems.at[count + p]) for p in range(count)
        ]
    for load in loads:
        load.start()

    def finish():
        lane = iota((TERMS, LANES), 1)
        for slot in range(49 * first, 49 * last):
            source = OFFSET_ROWS[slot]
            plane, inside = slot // 49 - first, slot % 49
            if inside == 0:
                loads[plane].wait()
            span = slice(inside * LANES, (inside + 1) * LANES)
            if source < 0:
                wide_ref[plane, :, span] = jnp.zeros((TERMS, LANES), BF16)
            else:
                base, shift = divmod(source * TERMS - start, LANES)
                merged = far_ref[:, base * LANES : (base + 1) * LANES]
                if shift + TERMS > LANES:
                    following = far_ref[:, (base + 1) * LANES : (base + 2) * LANES]
                    merged = jnp.where(lane >= shift, merged.astype(F32), following.astype(F32))
                    merged = merged.astype(BF16)
                if shift:
                    merged = pltpu.roll(merged, LANES - shift, 1)
                wide_ref[plane, :, span] = merged
            if inside == 48 and stores:
                stores[plane].start()
        for store in stores:
            store.wait()

    return finish


SPLITS = (0, 3, 6, 7)


def width_of(part):
    return CUTS[SPLITS[part + 1]] - max(CUTS[SPLITS[part]] - LANES, 0)


def first_kernel(far_hbm, after_ref, wide_hbm, far_ref, wide_ref, sems):
    widen(far_hbm, wide_hbm, far_ref, wide_ref, sems, SPLITS[0], SPLITS[1])()


def second_kernel(far_hbm, after_ref, wide_hbm, far_ref, wide_ref, sems):
    widen(far_hbm, wide_hbm, far_ref, wide_ref, sems, SPLITS[1], SPLITS[2])()


def write_picks(index_ref, upper_ref, child_ref):
    parity_x, parity_y, parity_z = index_ref[0], index_ref[1], index_ref[2]
    row = iota((256, LANES), 0)
    octant, box = row >> 5, row & 31
    vx = 2 * (box >> 3) + (octant >> 2) - parity_x
    vy = 2 * (box >> 2 & 1) + (octant >> 1 & 1) - parity_y
    vz = 2 * (box & 3) + (octant & 1) - parity_z
    write_hot(child_ref, spot(vx, vz, vy))
    row = iota((344, LANES), 0)
    plane = row * 1338 >> 16
    inside = row - plane * 49
    line = inside * 37 >> 8
    dx, dy, dz = plane - 3, line - 3, inside - line * 7 - 3
    fine = (dx >= -2 - parity_x) & (dx <= 3 - parity_x)
    fine = fine & (dy >= -2 - parity_y) & (dy <= 3 - parity_y)
    fine = fine & (dz >= -2 - parity_z) & (dz <= 3 - parity_z)
    write_hot(upper_ref, jnp.where(fine, spot(dx, dz, dy), -1))


def write_values(pos_ref, value_ref, mono):
    write_monomials(mono, (pos_ref[0], pos_ref[1], pos_ref[2]), None)
    for row in range(16):
        high, low = split(mono[pl.ds(row, LANES, stride=16), :])
        value_ref[0, :, row * LANES : (row + 1) * LANES] = high
        value_ref[1, :, row * LANES : (row + 1) * LANES] = low


VMEM_SPEC = pl.BlockSpec(memory_space=pltpu.VMEM)
HBM_SPEC = pl.BlockSpec(memory_space=pl.ANY)
SMEM_SPEC = pl.BlockSpec(memory_space=pltpu.SMEM)
WIDE = [jax.ShapeDtypeStruct((SPLITS[p + 1] - SPLITS[p], TERMS, PLANE), BF16) for p in range(3)]


def make_first():
    return pl.pallas_call(
        first_kernel,
        out_shape=WIDE[0],
        in_specs=[HBM_SPEC] * 2,
        out_specs=HBM_SPEC,
        scratch_shapes=[
            pltpu.VMEM((TERMS, width_of(0)), BF16),
            pltpu.VMEM(WIDE[0].shape, BF16),
            pltpu.SemaphoreType.DMA((6,)),
        ],
        name="first",
    )


def make_second():
    return pl.pallas_call(
        second_kernel,
        out_shape=WIDE[1],
        in_specs=[HBM_SPEC] * 2,
        out_specs=HBM_SPEC,
        scratch_shapes=[
            pltpu.VMEM((TERMS, width_of(1)), BF16),
            pltpu.VMEM(WIDE[1].shape, BF16),
            pltpu.SemaphoreType.DMA((6,)),
        ],
        name="second",
    )


def fill_window(window, left_ref, own_ref, right_ref, first_row):
    for bx in range(4):
        for by in range(4):
            for bz in range(4):
                if bx in (1, 2):
                    tile = own_ref[bx - 1, by, bz, first_row : first_row + 8, :]
                else:
                    at = 16 * (4 * by + bz) + first_row
                    tile = (left_ref if bx == 0 else right_ref)[at : at + 8, :]
                for i in range(2):
                    for j in range(2):
                        inner = i * 4 + j * 2
                        window[2 * bx + i, 2 * by + j, 2 * bz : 2 * bz + 2, :] = tile[inner : inner + 2, :]


def fill_slab(window, slab, tile, inner):
    for by in range(4):
        for bz in range(4):
            rows = tile(by, bz)
            for j in range(2):
                at = inner * 4 + j * 2
                window[slab, 2 * by + j, 2 * bz : 2 * bz + 2, :] = rows[at : at + 2, :]


def spread_slabs(window, rolled, spread, slabs, used):
    row8 = iota((8, LANES), 0)
    for x in range(slabs):
        for dz in range(3):
            for pair in range(3):
                first = pltpu.roll(window[x, 2 * pair + 1], 7 - dz, 0)
                second = pltpu.roll(window[x, 2 * pair + 2], (7 - dz + 4) % 8, 0)
                at = (x * 3 + dz) * 24 + 8 * pair
                rolled[at : at + 8, :] = jnp.where(row8 < 4, first, second)
    value = rolled[0 : used * 72, :]
    high = value.astype(BF16)
    rest = value - high.astype(F32)
    middle = rest.astype(BF16)
    low = (rest - middle.astype(F32)).astype(BF16)
    pieces = jnp.concatenate([high, middle, low], axis=1)
    column = iota((LANES, 2 * LANES), 1)
    row = iota((LANES, 2 * LANES), 0)
    for block in range(16):
        group, half = block // 2, block % 2
        wanted = (column // LANES + 2 * half) * SLOTS + 4 * group + column % LANES // SLOTS
        hot = (row == wanted).astype(F32).astype(BF16)
        found = jnp.dot(pieces, jnp.concatenate([hot, hot, hot], axis=0), preferred_element_type=F32)
        spread[2 * block] = found[:, 0:LANES]
        spread[2 * block + 1] = found[:, LANES : 2 * LANES]


def add_slab(mine, shift, spread, base, sums):
    tx = mine[0] - shift
    pot, fx, fy, fz = sums
    for ey in range(3):
        ty = mine[1] - float(ey - 1)
        for ez in range(3):
            tz = mine[2] - float(ez - 1)
            at = base + (ez * 24 + 4 * ey)
            for group in range(8):
                dx = tx - spread[4 * group, pl.ds(at, 16), :]
                dy = ty - spread[4 * group + 1, pl.ds(at, 16), :]
                dz = tz - spread[4 * group + 2, pl.ds(at, 16), :]
                inverse = lax.rsqrt(dx * dx + dy * dy + dz * dz + SOFTENING)
                weight = spread[4 * group + 3, pl.ds(at, 16), :] * inverse
                cubic = weight * (inverse * inverse)
                pot = pot + weight
                fx = fx + cubic * dx
                fy = fy + cubic * dy
                fz = fz + cubic * dz
    return pot, fx, fy, fz


def inner_kernel(own_ref, mine_ref, sum_ref, window, rolled, spread):
    for x in range(4):
        fill_slab(window, x, lambda by, bz: own_ref[x // 2, by, bz, 0:8, :], x % 2)
    spread_slabs(window, rolled, spread, 4, 3)
    slot = iota((16, LANES), 1) % SLOTS
    for x in range(4):
        own = rolled[(x * 3 + 1) * 24 + 4 : (x * 3 + 1) * 24 + 20, :]
        for c in range(4):
            mine_ref[x, c] = jnp.take_along_axis(own, c * SLOTS + slot, axis=1)
    sum_ref[...] = jnp.zeros((4, 4, 16, LANES), F32)

    def one_pair(step, carry):
        source = (step + 1) // 3
        shift = 1 - ((step + 1) - 3 * source)
        target = source - shift
        mine = [mine_ref[target, c] for c in range(3)]
        base = source * 72
        sums = tuple(sum_ref[target, c] for c in range(4))
        sums = add_slab(mine, shift.astype(F32), spread, base, sums)
        for c in range(4):
            sum_ref[target, c] = sums[c]
        return carry

    lax.fori_loop(0, 8, one_pair, 0)


def make_inner():
    return pl.pallas_call(
        inner_kernel,
        out_shape=(
            jax.ShapeDtypeStruct((4, 4, 16, LANES), F32),
            jax.ShapeDtypeStruct((4, 4, 16, LANES), F32),
        ),
        scratch_shapes=[
            pltpu.VMEM((4, 8, 8, LANES), F32),
            pltpu.VMEM((288, LANES), F32),
            pltpu.VMEM((32, 216, LANES), F32),
        ],
        compiler_params=pltpu.CompilerParams(vmem_limit_bytes=40 << 20),
        name="inner",
    )


def outer_kernel(left_ref, own_ref, right_ref, mine_ref, sum_ref, near_ref, sums_ref, window, rolled, spread):
    fill_slab(window, 0, lambda by, bz: left_ref[16 * (4 * by + bz) : 16 * (4 * by + bz) + 8, :], 1)
    fill_slab(window, 1, lambda by, bz: right_ref[16 * (4 * by + bz) : 16 * (4 * by + bz) + 8, :], 0)
    fill_slab(window, 2, lambda by, bz: own_ref[1, by, bz, 0:8, :], 1)
    spread_slabs(window, rolled, spread, 3, 3)
    sums_ref[...] = sum_ref[...]

    def one_pair(step, carry):
        target = jnp.where(step == 0, 0, jnp.where(step == 1, 2, 3))
        slab = jnp.where(step == 0, 0, jnp.where(step == 3, 1, 2))
        shift = jnp.where(step == 0, -1, jnp.where(step == 2, 0, 1))
        mine = [mine_ref[target, c] for c in range(3)]
        sums = tuple(sums_ref[target, c] for c in range(4))
        sums = add_slab(mine, shift.astype(F32), spread, slab * 72, sums)
        for c in range(4):
            sums_ref[target, c] = sums[c]
        return carry

    lax.fori_loop(0, 4, one_pair, 0)
    part = iota((16, LANES), 1) // SLOTS
    keep = part == iota((16, LANES), 0) % 4
    itself = lax.rsqrt(jnp.full((16, LANES), SOFTENING, F32))

    for x in range(4):
        totals = []
        for c in range(4):
            value = sums_ref[x, c]
            value = value + pltpu.roll(value, 64, 1)
            value = value + pltpu.roll(value, 32, 1)
            totals.append(value)
        totals[0] = totals[0] - mine_ref[x, 3] * itself
        for c in range(4):
            chosen = jnp.where(keep, totals[c], 0.0)
            rows = [jnp.sum(chosen[4 * y : 4 * y + 4], axis=0, keepdims=True) for y in range(4)]
            near_ref[c, x] = jnp.concatenate(rows, axis=0)


def make_outer():
    return pl.pallas_call(
        outer_kernel,
        out_shape=jax.ShapeDtypeStruct((4, 4, 4, LANES), F32),
        scratch_shapes=[
            pltpu.VMEM((4, 4, 16, LANES), F32),
            pltpu.VMEM((3, 8, 8, LANES), F32),
            pltpu.VMEM((216, LANES), F32),
            pltpu.VMEM((32, 216, LANES), F32),
        ],
        compiler_params=pltpu.CompilerParams(vmem_limit_bytes=40 << 20),
        name="outer",
    )


def two(value):
    return jnp.concatenate(split(value), axis=1)


def fetch_kernel(
    index_ref,
    far_hbm,
    first_hbm,
    second_hbm,
    pos_ref,
    pick_middle_ref,
    left_ref,
    own_ref,
    right_ref,
    middle_ref,
    after_ref,
    wide_first_ref,
    wide_second_ref,
    wide_third_ref,
    middle_rows,
    leaf_rows,
    value_ref,
    pick_upper_ref,
    pick_child_ref,
    window,
    rolled,
    mono,
    far_ref,
    sems,
):
    finish = widen(far_hbm, None, far_ref, wide_third_ref, sems, SPLITS[2], SPLITS[3])
    copies = [
        pltpu.make_async_copy(first_hbm, wide_first_ref, sems.at[1]),
        pltpu.make_async_copy(second_hbm, wide_second_ref, sems.at[2]),
    ]
    for copy in copies:
        copy.start()
    fill_window(window, left_ref, own_ref, right_ref, 8)
    row8 = iota((8, LANES), 0)
    row16 = iota((16, LANES), 0)
    rolled[:, 0:8, :] = jnp.zeros((7, 8, LANES), F32)
    rolled[:, 40:48, :] = jnp.zeros((7, 8, LANES), F32)

    def gather_plane(x, carry):
        for dz in range(-3, 4):
            for pair in range(4):
                even = pltpu.roll(window[x, 2 * pair], (16 - (dz + 2)) % 8, 0)
                odd = pltpu.roll(window[x, 2 * pair + 1], (16 - (dz + 2) + 4) % 8, 0)
                value = jnp.where(row8 < 4, even, odd)
                if dz == -3:
                    value = jnp.where(row8 % 2 == 1, value, 0.0)
                if dz == 3:
                    value = jnp.where(row8 % 2 == 0, value, 0.0)
                rolled[dz + 3, 8 + 8 * pair : 16 + 8 * pair, :] = value
        for dy in range(-3, 4):
            for dz in range(-3, 4):
                start = 8 + 4 * (dy + 2)
                value = rolled[dz + 3, start : start + 16, :]
                if dy == -3:
                    value = jnp.where(row16 // 4 % 2 == 1, value, 0.0)
                if dy == 3:
                    value = jnp.where(row16 // 4 % 2 == 0, value, 0.0)
                high, low = split(value)
                at = ((dy + 3) * 7 + dz + 3) * LANES
                leaf_rows[x, 0:16, at : at + LANES] = high
                leaf_rows[x, 16:32, at : at + LANES] = low
        return carry

    lax.fori_loop(0, 8, gather_plane, 0)
    middles = two(
        jnp.concatenate([left_ref[256:328, :], middle_ref[...], right_ref[256:328, :]], axis=0)
    )

    for p in range(7):
        found = jnp.dot(pick_middle_ref[392 * p : 392 * p + 392, :], middles, preferred_element_type=F32)
        for inside in range(49):
            piece = found[8 * inside : 8 * inside + 8]
            middle_rows[p, :, inside * LANES : (inside + 1) * LANES] = jnp.concatenate(
                [piece[:, 0:LANES], piece[:, LANES : 2 * LANES]], axis=0
            ).astype(BF16)
    write_picks(index_ref, pick_upper_ref, pick_child_ref)
    write_values(pos_ref, value_ref, mono)
    finish()
    for copy in copies:
        copy.wait()


FETCHED = (
    *WIDE,
    jax.ShapeDtypeStruct((7, 16, PLANE), BF16),
    jax.ShapeDtypeStruct((8, 32, PLANE), BF16),
    jax.ShapeDtypeStruct((2, LANES, 2048), BF16),
    jax.ShapeDtypeStruct((344, UPPER_ROWS), BF16),
    jax.ShapeDtypeStruct((256, UPPER_ROWS), BF16),
)


def make_fetch():
    return pl.pallas_call(
        fetch_kernel,
        out_shape=FETCHED,
        in_specs=[SMEM_SPEC] + [HBM_SPEC] * 3 + [VMEM_SPEC] * 6 + [HBM_SPEC],
        out_specs=(VMEM_SPEC,) * len(FETCHED),
        scratch_shapes=[
            pltpu.VMEM((8, 8, 8, LANES), F32),
            pltpu.VMEM((7, 48, LANES), F32),
            pltpu.VMEM((LANES * 16, LANES), F32),
            pltpu.VMEM((TERMS, width_of(2)), BF16),
            pltpu.SemaphoreType.DMA((3,)),
        ],
        compiler_params=pltpu.CompilerParams(vmem_limit_bytes=FETCH_LIMIT << 20),
        name="fetch",
    )


FETCH_LIMIT = 36


def far_kernel(
    index_ref,
    upper_left_ref,
    upper_own_ref,
    upper_right_ref,
    pick_top_ref,
    shift_ref,
    local_ref,
    lattice_ref,
    gradient_ref,
    near_ref,
    wide_first_ref,
    wide_second_ref,
    wide_third_ref,
    middle_rows,
    leaf_rows,
    value_ref,
    pick_upper_ref,
    pick_child_ref,
    live_ref,
    potential_ref,
    field_ref,
    few_rows,
    few,
    top,
    acc,
    local,
    shift_rows,
    local_rows,
):
    unpack_octants(shift_ref, shift_rows)
    unpack_octants(local_ref, local_rows)
    uppers = two(
        jnp.concatenate(
            [
                upper_left_ref[...],
                upper_own_ref[...],
                upper_right_ref[...],
                jnp.zeros((UPPER_ROWS - 648, LANES), F32),
            ],
            axis=0,
        )
    )
    children = jnp.dot(pick_child_ref[...], uppers, preferred_element_type=F32)
    total = jnp.zeros((32, TERMS), F32)
    for octant in range(8):
        rows = children[32 * octant : 32 * octant + 32]
        both = jnp.concatenate([rows[:, :TERMS], rows[:, LANES : LANES + TERMS]], axis=0).astype(BF16)
        made = nt_dot(both, octant_operator(shift_rows, octant))
        total = total + made[:32] + made[32:]
    top[...] = jnp.zeros((32, LANES), F32)
    top[:, 0:TERMS] = total
    few[...] = jnp.zeros((OFFSETS * 8 + 8, LANES), F32)
    from_upper = jnp.dot(pick_upper_ref[...], uppers, preferred_element_type=F32)
    from_top = jnp.dot(pick_top_ref[...], two(top[...]), preferred_element_type=F32)
    for side in range(2):
        span = slice(side * LANES, (side + 1) * LANES)
        few[pl.ds(2 * side, 344, stride=8), :] = from_upper[:, span]
        few[pl.ds(2 * side + 1, 344, stride=8), :] = from_top[:, span]
    none = jnp.zeros((8, LANES), F32)

    def few_plane(p):
        for inside in range(49):
            at = p * 392 + inside * 8
            few_rows[p, :, inside * LANES : (inside + 1) * LANES] = jnp.concatenate(
                [few[at : at + 8, :], none], axis=0
            ).astype(BF16)

    acc[...] = jnp.zeros((160, LANES), F32)
    for p in range(7):
        few_plane(p)
        if p == 0:
            parts, places = [0, 2], [1, 3]
        elif p == 6:
            parts, places = [5, 7], [0, 2]
        else:
            parts, places = None, None
        if parts is None:
            left = leaf_rows[p - 1 : p + 3].reshape(128, PLANE)
        else:
            left = jnp.concatenate([leaf_rows[q] for q in parts], axis=0)
        left = jnp.concatenate([left, middle_rows[p], few_rows[p]], axis=0)
        part = p // 3
        right = (wide_first_ref, wide_second_ref, wide_third_ref)[part][p - SPLITS[part]]
        found = nt_dot(left, right)
        if parts is None:
            acc[:, 0:TERMS] += found
        else:
            for n, place in enumerate(places):
                acc[32 * place : 32 * place + 32, 0:TERMS] += found[32 * n : 32 * n + 32]
            acc[128:160, 0:TERMS] += found[64:96]

    far_middle = acc[128:136, :] + acc[136:144, :]
    far_rest = acc[144:146, :] + acc[146:148, :]
    root = jnp.sum(top[...], axis=0, keepdims=True)
    local[...] = jnp.zeros((8, LANES), F32)
    lattice = apply_op(jnp.broadcast_to(root, (8, LANES)), lattice_ref[...])
    local[:, 0:TERMS] = 0.125 * (far_rest[1:2, 0:TERMS] + lattice)
    own = index_ref[0] * 4 + index_ref[1] * 2 + index_ref[2]
    lowered = apply_op(local[...], octant_operator(local_rows, own))
    local[:, 0:TERMS] = 0.25 * far_rest[0:1, 0:TERMS] + lowered
    row_terms = iota((8, TERMS), 0)
    upper_local = local[...]
    spread = jnp.zeros((8, TERMS), F32)
    for octant in range(8):
        spread = spread + jnp.where(row_terms == octant, apply_op(upper_local, octant_operator(local_rows, octant)), 0.0)
    local[:, 0:TERMS] = 0.5 * far_middle[:, 0:TERMS] + spread
    middle_local = local[...]
    for x in range(4):
        base = 32 * x
        acc[base : base + 16, :] = acc[base : base + 16, :] + acc[base + 16 : base + 32, :]
    for octant in range(8):
        i, j, l = octant >> 2, octant >> 1 & 1, octant & 1
        made = apply_op(middle_local, octant_operator(local_rows, octant))
        for parent in range(8):
            bx, by, bz = parent >> 2, parent >> 1 & 1, parent & 1
            at = 32 * (2 * bx + i) + 4 * (2 * by + j) + 2 * bz + l
            acc[at : at + 1, 0:TERMS] += made[parent : parent + 1]
    for x in range(4):
        base = acc[32 * x : 32 * x + 16, :]
        high, low = split(base)
        both = jnp.concatenate([high, low], axis=0)
        listed = [base]
        for axis in range(3):
            made = jnp.dot(both, gradient_ref[axis], preferred_element_type=F32)
            listed.append(-(made[:16] + made[16:]))
        high, low = split(jnp.concatenate(listed, axis=0))
        first = value_ref[0, :, 512 * x : 512 * x + 512]
        second = value_ref[1, :, 512 * x : 512 * x + 512]
        found = jnp.dot(jnp.concatenate([high, low], axis=0), first, preferred_element_type=F32)
        found = found[:64] + found[64:] + jnp.dot(high, second, preferred_element_type=F32)
        keep = iota((4, LANES), 1) // SLOTS == iota((4, LANES), 0)
        for c in range(4):
            rows = []
            for y in range(4):
                piece = found[16 * c + 4 * y : 16 * c + 4 * y + 4, LANES * y : LANES * y + LANES]
                rows.append(jnp.sum(jnp.where(keep, piece, 0.0), axis=0, keepdims=True))
            value = (near_ref[c, x] + jnp.concatenate(rows, axis=0)) * live_ref[4 * x : 4 * x + 4, :]
            if c == 0:
                potential_ref[x] = value
            else:
                field_ref[c - 1, x] = value


def make_far():
    return pl.pallas_call(
        far_kernel,
        out_shape=(
            jax.ShapeDtypeStruct((4, 4, LANES), F32),
            jax.ShapeDtypeStruct((3, 4, 4, LANES), F32),
        ),
        in_specs=[SMEM_SPEC] + [VMEM_SPEC] * 18,
        scratch_shapes=[
            pltpu.VMEM((7, 16, PLANE), BF16),
            pltpu.VMEM((OFFSETS * 8 + 8, LANES), F32),
            pltpu.VMEM((32, LANES), F32),
            pltpu.VMEM((160, LANES), F32),
            pltpu.VMEM((8, LANES), F32),
            pltpu.VMEM((8 * TERMS, LANES), F32),
            pltpu.VMEM((8 * TERMS, LANES), F32),
        ],
        compiler_params=pltpu.CompilerParams(vmem_limit_bytes=24 << 20),
        name="far",
    )


def shifted(value, axis, shift):
    count = lax.axis_size(axis)
    return lax.ppermute(value, axis, [(i, (i + shift) % count) for i in range(count)])


def selections():
    slots = np.arange(344)
    dx = np.minimum(slots // 49, 6) - 3
    dy = slots // 7 % 7 - 3
    dz = slots % 7 - 3
    parent = np.arange(8)
    px, py, pz = parent >> 2, parent >> 1 & 1, parent & 1
    wide = [d[:, None] + p[None, :] + 2 for d, p in ((dx, px), (dy, py), (dz, pz))]
    fine = np.ones((344, 8), bool)
    for d, p in ((dx, px), (dy, py), (dz, pz)):
        fine &= (d[:, None] >= -2 - p[None, :]) & (d[:, None] <= 3 - p[None, :])
    column = ((wide[0] // 2 * 3 + wide[2] // 2) * 3 + wide[1] // 2) * 8
    column = column + wide[0] % 2 * 4 + wide[1] % 2 * 2 + wide[2] % 2
    middle = np.where(fine, column, -1).reshape(-1)
    top = ((dx % 4) * 2 + dy % 2) * 4 + dz % 4
    hot = [
        (place[:, None] == np.arange(width)[None, :]).astype(np.float32).astype(jnp.bfloat16)
        for place, width in ((middle, 216), (top, 32))
    ]
    return jnp.asarray(hot[0]), jnp.asarray(hot[1])


def per_device(positions, charges, counts, moment_shift, far_operators, local_shift, lattice_operator):
    index = jnp.stack([lax.axis_index(axis) % 2 for axis in ("gx", "gy", "gz")]).astype(jnp.int32)
    pos = positions.reshape(3, 16, LANES)
    shift = moment_shift.transpose(1, 0, 2)
    local = local_shift.transpose(1, 0, 2)
    comb, low, high, middle, alone, live = make_moments()(
        pos, charges.reshape(16, LANES), counts.reshape(16, 4), shift
    )
    pick_middle, pick_top = selections()

    def exchange(axis, low, high):
        return shifted(high, axis, 1), shifted(low, axis, -1)

    def pack(block, *rest):
        return jnp.concatenate([block.reshape(-1, LANES), *rest], axis=0)

    left, right = exchange("gy", low, high)
    above = shifted(alone, "gy", -2)
    near_copy = jnp.concatenate([comb.reshape(LANES, LANES), middle, alone], axis=0)
    near_copy = lax.optimization_barrier(near_copy)
    wide_first = make_first()(far_operators, alone)
    blocks = near_copy[:128].reshape(2, 2, 2, 16, LANES)
    middle, alone = near_copy[128:136], near_copy[136:144]
    sides = [left[:64].reshape(2, 1, 2, 16, LANES), right[:64].reshape(2, 1, 2, 16, LANES)]
    blocks = jnp.concatenate([sides[0], blocks, sides[1]], axis=1)
    middle = jnp.concatenate([left[64:72], middle, right[64:72]], axis=0)
    line = jnp.concatenate(
        [left[72:73], alone[0:1], right[72:73], above[0:1], jnp.zeros((4, LANES), F32)], axis=0
    )

    sends = (pack(blocks[:, :, 0], middle, line), pack(blocks[:, :, 1], middle, line))
    sends, blocks, middle, line, wide_first = lax.optimization_barrier(
        (sends, blocks, middle, line, wide_first)
    )
    left, right = exchange("gz", *sends)
    wide_second = make_second()(far_operators, wide_first)
    sides = [left[:128].reshape(2, 4, 1, 16, LANES), right[:128].reshape(2, 4, 1, 16, LANES)]
    blocks = jnp.concatenate([sides[0], blocks, sides[1]], axis=2)
    middle = jnp.concatenate([left[128:152], middle, right[128:152]], axis=0)
    line = jnp.concatenate([left[152:160], line, right[152:160]], axis=0)

    sends = (pack(blocks[0], middle, line), pack(blocks[1], middle, line))
    sends, blocks, middle, line, wide_second = lax.optimization_barrier(
        (sends, blocks, middle, line, wide_second)
    )
    left, right = exchange("gx", *sends)
    mine, sums = make_inner()(blocks)

    sheet = jnp.concatenate([left[328:352], line, right[328:352]], axis=0)
    sheet, sums = lax.optimization_barrier((sheet, sums))
    sheet = jnp.concatenate([shifted(sheet, "gz", 3), sheet, shifted(sheet, "gz", -3)], axis=0)
    near = make_outer()(left, blocks, right, mine, sums)
    sheet, near = lax.optimization_barrier((sheet, near))
    upper_left = shifted(sheet, "gx", 3)
    upper_right = shifted(sheet, "gx", -3)

    prepared = make_fetch()(
        index, far_operators, wide_first, wide_second, pos, pick_middle, left, blocks, right, middle, near
    )
    gradients = jnp.asarray(gradient_tables(), BF16)
    return make_far()(
        index,
        upper_left,
        sheet,
        upper_right,
        pick_top,
        shift,
        local,
        lattice_operator,
        gradients,
        near,
        *prepared,
        live,
    )


def solution(mesh):
    placed = (
        P(None, "gx", "gy", "gz"),
        P("gx", "gy", "gz"),
        P("gx", "gy", "gz"),
        P(),
        P(),
        P(),
        P(),
    )
    return jax.shard_map(
        per_device,
        mesh=mesh,
        in_specs=placed,
        out_specs=(P("gx", "gy", "gz"), P(None, "gx", "gy", "gz")),
        check_vma=False,
    )
```
